32 devices in a mesh: prow: 4 (over x, core), pcol: 8 (over z, y).
Axes of the slice: x: 2, y: 2, z: 4, core: 2. Of those that a mesh axis runs over, the one named last changes fastest.
Arguments:
- matrix: float32 [4, 8, 768, 384], P('prow', 'pcol'), may hold values from -6 to 6
- pivots: int32 [3, 384], replicated, may hold values from 0 to 3071, as said below
- lower_inv: float32 [3, 384, 384], replicated, may hold values from -0.3125 to 0.3125
- upper_inv: float32 [3, 384, 384], replicated, may hold values from -0.015625 to 0.015625
Outputs:
- factored: float32 [4, 8, 768, 384], P('prow', 'pcol')
The draws below stay inside these ranges and needn't reach their ends.
Inputs may be any that keep to these rules, and one draw needn't show every extreme that they name: Within one step s the indices pivots[s, i] are distinct, and each equals s * 384 + i or lies between (s + 1) * 384 and 3071.
All inputs are finite; a program needn't handle non-finite values.
Results may differ from the reference program's by a relative error of at most 0.0002.
Values sent between devices are 32-bit elements; how exact they have to be, the bound alone decides.
A program may use at most 64 MiB of HBM per device.

```python
import jax
import jax.numpy as jnp
from jax import lax

NB = 384
ROWB = 2
STEPS = 3
ORDER = 3072
COLB = 1
N_PROW = 4
N_PCOL = 8


def draw_pivots(key, part):
    offsets = jnp.arange(NB, dtype=jnp.int32)
    listed = []
    for section in range(STEPS):
        section_key = jax.random.fold_in(key, 7919 + section)
        first = section * NB
        finish = first + NB
        shuffled = jax.random.permutation(jax.random.fold_in(section_key, 1), ORDER - finish)[:NB].astype(jnp.int32) + finish
        staying = jax.random.randint(jax.random.fold_in(section_key, 2), (NB,), 0, 4, dtype=jnp.int32) == 0
        listed.append(jnp.where(staying, first + offsets, shuffled).astype(jnp.int32))
    return jnp.stack(listed).astype(jnp.int32)


def steps_of(rng, shape, shards, low, high):
    gain = 1.0
    for axis_at, parts in shards:
        steps = jax.random.uniform(jax.random.fold_in(jax.random.fold_in(rng, 6), axis_at), (parts,), jnp.float32, low / len(shards), high / len(shards))
        gain = gain * jnp.repeat(jnp.exp(steps), shape[axis_at] // parts).reshape((-1,) + (1,) * (len(shape) - 1 - axis_at))
    return gain


def centred(key, extent, scale, bound, cuts=(), kind=jnp.bfloat16):
    drawn = jax.random.normal(key, extent, jnp.float32) * scale
    if len(cuts) > 0:
        drawn = steps_of(key, extent, cuts, -0.22, 0.18) * drawn
    return jnp.clip(drawn, min=-bound, max=bound).astype(kind)


def setup_inputs(seed: int = 0) -> dict:
    arg_keys = jax.random.split(jax.random.key(seed), 5)
    matrix = centred(arg_keys[0], (N_PROW, N_PCOL, ROWB * NB, COLB * NB), 1.0, 6.0, ((0, 4), (1, 8)), jnp.float32)
    pivots = draw_pivots(jax.random.fold_in(arg_keys[4], 71), 0)
    lower_inv = centred(arg_keys[2], (STEPS, NB, NB), NB ** -0.5, 0.3125, (), jnp.float32)
    upper_inv = centred(arg_keys[3], (STEPS, NB, NB), (NB * NB) ** -0.5, 0.015625, (), jnp.float32)
    return dict(matrix=matrix, pivots=pivots, lower_inv=lower_inv, upper_inv=upper_inv)


def compose(pivot_list, first):
    identity = jnp.arange(ORDER, dtype=jnp.int32)

    def exchange_pair(position, permutation):
        target = (first + position).astype(jnp.int32)
        source = pivot_list[position]
        held_here = permutation[target]
        held_there = permutation[source]
        return permutation.at[target].set(held_there).at[source].set(held_here)

    return lax.fori_loop(0, NB, exchange_pair, identity)


def reference(matrix, pivots, lower_inv, upper_inv):
    precise = lax.Precision.HIGHEST
    whole = matrix.reshape(N_PROW, N_PCOL, ROWB, NB, COLB, NB).transpose(2, 0, 3, 4, 1, 5).reshape(ORDER, ORDER)
    offsets = jnp.arange(NB, dtype=jnp.int32)
    for section in range(STEPS):
        start = section * NB
        finish = start + NB
        pivot_list = pivots[section]
        permutation = compose(pivot_list, start)
        targets = jnp.concatenate([(start + offsets).astype(jnp.int32), pivot_list.astype(jnp.int32)])
        sources = permutation[targets]
        whole = whole.at[targets].set(whole[sources])
        lower_unit = jnp.eye(NB, dtype=jnp.float32) + jnp.tril(lower_inv[section], -1)
        upper_tri = jnp.triu(upper_inv[section])
        upper_rows = jnp.dot(lower_unit, whole[start:finish, finish:], precision=precise, preferred_element_type=jnp.float32)
        lower_panel = jnp.dot(whole[finish:, start:finish], upper_tri, precision=precise, preferred_element_type=jnp.float32)
        whole = whole.at[start:finish, finish:].set(upper_rows)
        whole = whole.at[finish:, start:finish].set(lower_panel)
        update = jnp.dot(lower_panel, upper_rows, precision=precise, preferred_element_type=jnp.float32)
        whole = whole.at[finish:, finish:].set(whole[finish:, finish:] - update)
    return whole.reshape(ROWB, N_PROW, NB, COLB, N_PCOL, NB).transpose(1, 4, 0, 2, 3, 5).reshape(N_PROW, N_PCOL, ROWB * NB, COLB * NB)
```

```python
import functools

import jax
import jax.numpy as jnp
from jax import lax
from jax.experimental import pallas as pl
from jax.experimental.pallas import tpu as pltpu
from jax.sharding import PartitionSpec as P

MESH = pl.DeviceIdType.MESH
CORES = 2
F32 = jnp.float32
BF16 = jnp.bfloat16
HOP = 2


def grid_width(count):
    width = 1
    while (2 * width) * (2 * width) <= count:
        width *= 2
    return width if count % width == 0 else 1


def both(*conds):
    out = conds[0]
    for cond in conds[1:]:
        out = jnp.logical_and(out, cond)
    return out


def entry_barrier(neighbours):
    barrier = pltpu.get_barrier_semaphore()
    total = jnp.int32(0)
    for cond, device in neighbours:
        total = total + jnp.where(cond, 1, 0).astype(jnp.int32)

        @pl.when(cond)
        def _(device=device):
            pl.semaphore_signal(barrier, inc=1, device_id=device, device_id_type=MESH)

    pl.semaphore_wait(barrier, total)


def line_ways(prow, prow_count):
    x, core = prow // CORES, prow % CORES
    chips = prow_count // CORES
    return [
        (x + 1 < chips, {"prow": prow + CORES}),
        (x > 0, {"prow": prow - CORES}),
        (prow >= 0, {"prow": x * CORES + (CORES - 1 - core)}),
    ]


def line_sends(prow, prow_count, source):
    x, core = prow // CORES, prow % CORES
    ways = line_ways(prow, prow_count)
    sx, sc = source // CORES, source % CORES
    return [
        (both(ways[0][0], core == sc, x >= sx), ways[0][1]),
        (both(ways[1][0], core == sc, x <= sx), ways[1][1]),
        (core == sc, ways[2][1]),
    ]


def grid_ways(pcol, pcol_count):
    width = grid_width(pcol_count)
    height = pcol_count // width
    z, y = pcol // width, pcol % width
    return [
        (z + 1 < height, {"pcol": pcol + width}),
        (z > 0, {"pcol": pcol - width}),
        (y + 1 < width, {"pcol": pcol + 1}),
        (y > 0, {"pcol": pcol - 1}),
    ]


def tree_sends(pcol, pcol_count, source, first_axis):
    width = grid_width(pcol_count)
    height = pcol_count // width
    ways = grid_ways(pcol, pcol_count)
    pos = (pcol // width, pcol % width)
    src = (source // width, source % width)
    extent = (height, width)
    a, b = first_axis, 1 - first_axis
    away = {0: ways[0:2], 1: ways[2:4]}
    near = src[a] + 1 if src[a] + 1 < extent[a] else src[a] - 1
    trunk = pos[b] == src[b]
    off_row = pos[a] != src[a]
    sends = {}
    if extent[a] == 1:
        sends[a] = [pos[a] < 0, pos[a] < 0]
        sends[b] = [pos[b] >= src[b], pos[b] <= src[b]]
    else:
        back_up = both(pos[a] == near, jnp.logical_not(trunk))
        up = both(trunk, pos[a] >= src[a])
        down = both(trunk, pos[a] <= src[a])
        if near > src[a]:
            down = jnp.logical_or(down, back_up)
        else:
            up = jnp.logical_or(up, back_up)
        sends[a] = [up, down]
        sends[b] = [both(off_row, pos[b] >= src[b]), both(off_row, pos[b] <= src[b])]
    out = []
    for axis in (0, 1):
        for way in (0, 1):
            out.append((both(away[axis][way][0], sends[axis][way]), away[axis][way][1]))
    return out


def tree_hops(pcol, pcol_count, source, first_axis):
    width = grid_width(pcol_count)
    extent = (pcol_count // width, width)
    pos = (pcol // width, pcol % width)
    src = (source // width, source % width)
    a, b = first_axis, 1 - first_axis
    straight = jnp.abs(pos[a] - src[a]) + jnp.abs(pos[b] - src[b])
    if extent[a] == 1:
        return straight
    return straight + jnp.where(both(pos[a] == src[a], pos[b] != src[b]), 2, 0)


class Flow:
    def __init__(self, mine, start_ref, land_ref, sends, send_sem, recv_sem, rows):
        self.mine, self.start_ref, self.land_ref = mine, start_ref, land_ref
        self.sends, self.send_sem, self.recv_sem, self.rows = sends, send_sem, recv_sem, rows

    def copy(self, chunk, way, ref):
        piece = pl.ds(chunk * self.rows, self.rows)
        return pltpu.make_async_remote_copy(
            src_ref=ref.at[piece],
            dst_ref=self.land_ref.at[piece],
            send_sem=self.send_sem.at[way, chunk],
            recv_sem=self.recv_sem.at[chunk],
            device_id=self.sends[way][1],
            device_id_type=MESH,
        )

    def send(self, chunk, ref):
        for way, (cond, _device) in enumerate(self.sends):

            @pl.when(cond)
            def _(way=way):
                self.copy(chunk, way, ref).start()

    def pass_on(self, chunk):
        @pl.when(jnp.logical_not(self.mine))
        def _():
            self.copy(chunk, 0, self.land_ref).wait_recv()
            self.send(chunk, self.land_ref)

    def finish(self, chunk):
        for way, (cond, _device) in enumerate(self.sends):

            @pl.when(cond)
            def _(way=way):
                self.copy(chunk, way, self.land_ref).wait_send()


def split2(value):
    high = value.astype(BF16)
    low = (value - high.astype(F32)).astype(BF16)
    return high, low


def split3(value):
    high = value.astype(BF16)
    rest = value - high.astype(F32)
    middle = rest.astype(BF16)
    low = (rest - middle.astype(F32)).astype(BF16)
    return high, middle, low


def wide(value):
    high, low = split2(value)
    return jnp.concatenate([high, high, low], axis=1)


def dot(left, right):
    return jnp.dot(left, right, preferred_element_type=F32)


def factor_kernel(
    prow_count, pcol_count, sections, width, blocks,
    tile_ref, pivots_ref, lower_ref, upper_ref, out_ref,
    first, pivot, low_in, up_in, parts, top, top_parts, picked, picked_in,
    row_panel, col_panel, row_stack, low_wide, up_stack, core_stack,
    local_sem, top_send, top_recv, pick_send, pick_recv,
    row_send, row_recv, col_send, col_recv,
):
    prow = lax.axis_index("prow")
    pcol = lax.axis_index("pcol")
    x, core = prow // CORES, prow % CORES
    chips = prow_count // CORES
    step_rows = width // 3
    tiles = width // step_rows
    relay_rows = col_panel.shape[1] // (2 * col_recv.shape[2])
    span = 2 * relay_rows
    per_block = width // span

    load_tile = pltpu.make_async_copy(tile_ref, first, local_sem.at[0])
    load_pivots = pltpu.make_async_copy(pivots_ref, pivot, local_sem.at[1])
    load_pivots.start()
    load_tile.start()
    owns_row = prow < sections
    owns_col = pcol < sections

    @pl.when(owns_row)
    def _():
        pltpu.make_async_copy(lower_ref.at[prow], low_in, local_sem.at[2]).start()

    @pl.when(owns_col)
    def _():
        pltpu.make_async_copy(upper_ref.at[pcol], up_in, local_sem.at[3]).start()

    top_flows = [
        Flow(
            prow == s, tile_ref, top.at[pl.ds(s * width, width)],
            line_sends(prow, prow_count, s), top_send.at[s], top_recv.at[s], step_rows,
        )
        for s in range(sections)
    ]
    row_flows = [
        Flow(
            prow == s, row_panel.at[s], row_panel.at[s],
            line_sends(prow, prow_count, s), row_send.at[s], row_recv.at[s], step_rows,
        )
        for s in range(sections)
    ]

    entry_barrier(line_ways(prow, prow_count) + grid_ways(pcol, pcol_count))

    for s in range(sections):

        @pl.when(prow == s)
        def _(s=s):
            for chunk in range(tiles):
                top_flows[s].send(chunk, tile_ref)
            pltpu.make_async_copy(
                tile_ref.at[pl.ds(0, width)], top.at[pl.ds(s * width, width)], local_sem.at[4]
            ).start()

    def lanes(count):
        return lax.broadcasted_iota(jnp.int32, (1, count), 1).astype(F32)

    def column(start):
        ids = lax.broadcasted_iota(jnp.int32, (step_rows, 1), 0)
        return (ids + start).astype(F32)

    def pivot_row(s):
        return pivot[pl.ds(s, 1), :].astype(F32)

    def undo(rows, upto):
        for s in reversed(range(upto)):
            listed = pivot_row(s)
            shift = lanes(width) + F32(s * width) - listed
            moved = jnp.where(rows == listed, shift, F32(0))
            rows = rows + jnp.sum(moved, axis=1, keepdims=True)
        return rows

    def one_hot(rows, ids):
        return jnp.where(rows == ids, F32(1), F32(0)).astype(BF16)

    load_pivots.wait()
    load_tile.wait()

    def cut_tile(i, carry):
        at = pl.ds(pl.multiple_of(i * step_rows, step_rows), step_rows)
        for k, part in enumerate(split3(first[at, :])):
            parts[k, at, :] = part
        return carry

    lax.fori_loop(0, tiles * blocks, cut_tile, 0)

    def pick_copy(s, slot, where, device):
        return pltpu.make_async_remote_copy(
            src_ref=picked.at[s],
            dst_ref=picked_in.at[s, slot],
            send_sem=pick_send.at[s, where],
            recv_sem=pick_recv.at[s, slot],
            device_id=device,
            device_id_type=MESH,
        )

    partner = {"prow": x * CORES + (CORES - 1 - core)}
    held_ids = jnp.concatenate(
        [
            lanes(width) + ((block * prow_count + prow) * width).astype(F32)
            for block in range(blocks)
        ],
        axis=1,
    )
    for s in range(sections):

        def pick(i, carry, s=s):
            start = i * step_rows
            at = pl.ds(pl.multiple_of(start, step_rows), step_rows)
            rows = jnp.sum(
                jnp.where(column(start) == lanes(width), pivot_row(s), F32(0)),
                axis=1, keepdims=True,
            )
            chosen = one_hot(undo(rows, s), held_ids)
            picked[s, at, :] = (
                dot(chosen, parts[2]) + dot(chosen, parts[1]) + dot(chosen, parts[0])
            )
            return carry

        lax.fori_loop(0, tiles, pick, 0)

        @pl.when(core != s % CORES)
        def _(s=s):
            pick_copy(s, 0, 0, partner).start()

    def add_in(s, slot):
        pick_copy(s, slot, 1, partner).wait_recv()

        def add(i, carry):
            at = pl.ds(pl.multiple_of(i * step_rows, step_rows), step_rows)
            picked[s, at, :] += picked_in[s, slot, at, :]
            return carry

        lax.fori_loop(0, tiles, add, 0)

    def pass_picked(s, when):
        owner = s // CORES

        @pl.when(both(core == s % CORES, x != owner, when))
        def _():
            add_in(s, 0)

            @pl.when(both(x < owner, x > 0))
            def _():
                add_in(s, 1)

            @pl.when(both(x > owner, x < chips - 1))
            def _():
                add_in(s, 2)

            @pl.when(x < owner)
            def _():
                pick_copy(s, 1, 1, {"prow": prow + CORES}).start()

            @pl.when(x > owner)
            def _():
                pick_copy(s, 2, 1, {"prow": prow - CORES}).start()

    def urgent(s):
        return pcol > 0 if s == 0 else pcol == 0

    for s in range(sections):
        pass_picked(s, urgent(s))

    @pl.when(owns_row)
    def _():
        pltpu.make_async_copy(lower_ref.at[prow], low_in, local_sem.at[2]).wait()

        def prepare(i, carry):
            start = i * step_rows
            at = pl.ds(pl.multiple_of(start, step_rows), step_rows)
            below = column(start) > lanes(width)
            same = column(start) == lanes(width)
            unit = jnp.where(below, low_in[at, :], jnp.where(same, F32(1), F32(0)))
            low_wide[at, :] = wide(unit)
            return carry

        lax.fori_loop(0, tiles, prepare, 0)

    def stack(ref, i, value):
        high, low = split2(value)
        start = i * step_rows
        for k, part in enumerate((high, low, high)):
            at = pl.ds(pl.multiple_of(k * width + start, step_rows), step_rows)
            ref[at, :] = part

    @pl.when(owns_col)
    def _():
        pltpu.make_async_copy(upper_ref.at[pcol], up_in, local_sem.at[3]).wait()

        def prepare(i, carry):
            start = i * step_rows
            at = pl.ds(pl.multiple_of(start, step_rows), step_rows)
            kept = jnp.where(column(start) <= lanes(width), up_in[at, :], F32(0))
            stack(up_stack, i, kept)
            return carry

        lax.fori_loop(0, tiles, prepare, 0)

    for chunk in range(tiles):
        for flow in top_flows:
            flow.pass_on(chunk)
    for s in range(sections):

        @pl.when(prow == s)
        def _(s=s):
            pltpu.make_async_copy(
                tile_ref.at[pl.ds(0, width)], top.at[pl.ds(s * width, width)], local_sem.at[4]
            ).wait()

    def take_picked(s):
        owner = s // CORES
        add_in(s, 0)
        if owner > 0:
            add_in(s, 1)
        if owner < chips - 1:
            add_in(s, 2)
        out_ref[pl.ds(0, width), :] = picked[s]

    def row_product(s):
        def cut(i, carry):
            at = pl.ds(pl.multiple_of(i * step_rows, step_rows), step_rows)
            stack(core_stack, i, out_ref[at, :])
            return carry

        lax.fori_loop(0, tiles, cut, 0)
        for chunk in range(tiles):
            at = pl.ds(chunk * step_rows, step_rows)
            value = dot(low_wide[at, :], core_stack[...])
            row_panel[s, at, :] = value
            out_ref[at, :] = value
            if chunk > 0:
                row_flows[s].send(chunk - 1, row_panel.at[s])
        row_flows[s].send(tiles - 1, row_panel.at[s])

    @pl.when(both(prow == 0, pcol > 0))
    def _():
        take_picked(0)
        row_product(0)

    for s in range(sections):
        pass_picked(s, jnp.logical_not(urgent(s)))

    def cut_top(i, carry):
        at = pl.ds(pl.multiple_of(i * step_rows, step_rows), step_rows)
        for k, part in enumerate(split3(top[at, :])):
            top_parts[k, at, :] = part
        return carry

    lax.fori_loop(0, tiles * sections, cut_top, 0)

    def settle(block):
        def place(i, carry):
            start = i * step_rows
            at = pl.ds(pl.multiple_of(block * width + start, step_rows), step_rows)
            rows = column(start + (block * prow_count + prow) * width)
            rows = undo(rows, sections)
            chosen = one_hot(rows, lanes(sections * width))
            value = (
                dot(chosen, top_parts[2]) + dot(chosen, top_parts[1]) + dot(chosen, top_parts[0])
            )
            out_ref[at, :] = jnp.where(rows < F32(sections * width), value, first[at, :])
            return carry

        lax.fori_loop(0, tiles, place, 0)

    for block in range(1, blocks):
        settle(block)

    @pl.when(jnp.logical_not(owns_row))
    def _():
        settle(0)

    sends = [
        [tree_sends(pcol, pcol_count, s, k) for k in range(2)] for s in range(sections)
    ]

    def live(s):
        return jnp.where(prow > s, blocks, blocks - 1)

    def place_of(s, i):
        turn = lax.div(i, per_block)
        block = blocks - 1 - turn if s == 0 else blocks - live(s) + turn
        return block * width + (i - turn * per_block) * span

    def col_copy(s, k, i, way):
        start = pl.multiple_of(place_of(s, i) + k * relay_rows, relay_rows)
        piece = pl.ds(start, relay_rows)
        return pltpu.make_async_remote_copy(
            src_ref=col_panel.at[s, piece],
            dst_ref=col_panel.at[s, piece],
            send_sem=col_send.at[s, k, way, i],
            recv_sem=col_recv.at[s, k, i],
            device_id=sends[s][k][way][1],
            device_id_type=MESH,
        )

    def col_start(s, k, i):
        for way in range(4):

            @pl.when(sends[s][k][way][0])
            def _(way=way):
                col_copy(s, k, i, way).start()

    def update(s, at):
        return out_ref[at, :] - dot(wide(col_panel[s, at, :]), row_stack[...])

    def produce(s, start, stop, updated):
        def body(i, carry):
            at = pl.ds(pl.multiple_of(place_of(s, i), span), span)
            value = update(s - 1, at) if updated else out_ref[at, :]
            value = dot(wide(value), up_stack[...])
            col_panel[s, at, :] = value
            out_ref[at, :] = value

            @pl.when(i > start)
            def _():
                for k in range(2):
                    col_start(s, k, i - 1)

            return carry

        lax.fori_loop(start, stop, body, 0)
        for k in range(2):
            col_start(s, k, stop - 1)

    def relay(s, hook):
        hops = [tree_hops(pcol, pcol_count, s, k) for k in range(2)]
        late = [HOP * jnp.maximum(hops[k] - hops[1 - k], 0) for k in range(2)]
        count = live(s) * per_block

        def body(t, carry):
            for k in range(2):
                i = t - late[k]

                @pl.when(both(i >= 0, i < count))
                def _(k=k, i=i):
                    col_copy(s, k, i, 0).wait_recv()
                    col_start(s, k, i)

            return carry

        lax.fori_loop(0, per_block, body, 0)
        hook()
        lax.fori_loop(per_block, count + late[0] + late[1], body, 0)

    def update_block(s, block):
        def body(i, carry):
            at = pl.ds(pl.multiple_of(block * width + i * step_rows, step_rows), step_rows)
            out_ref[at, :] = update(s, at)
            return carry

        lax.fori_loop(0, tiles, body, 0)

    @pl.when(pcol == 0)
    def _():
        produce(0, 0, (blocks - 1) * per_block, False)
        for s in range(sections):

            @pl.when(prow == s)
            def _(s=s):
                take_picked(s)

        @pl.when(prow > 0)
        def _():
            produce(0, (blocks - 1) * per_block, blocks * per_block, False)

    for s in range(sections):

        @pl.when(pcol != s)
        def _(s=s):
            def hook():
                @pl.when(pcol > s)
                def _():
                    for chunk in range(tiles):
                        row_flows[s].pass_on(chunk)

            relay(s, hook)

        @pl.when(pcol > s)
        def _(s=s):
            if s == 0:
                for other in range(1, sections):

                    @pl.when(prow == other)
                    def _(other=other):
                        take_picked(other)

            def cut(i, carry):
                at = pl.ds(pl.multiple_of(i * step_rows, step_rows), step_rows)
                stack(row_stack, i, row_panel[s, at, :])
                return carry

            lax.fori_loop(0, tiles, cut, 0)
            last = s + 1 == sections

            def plain():
                @pl.when(prow > s)
                def _():
                    update_block(s, 0)

                if not last:

                    @pl.when(prow == s + 1)
                    def _():
                        row_product(s + 1)

                for block in range(1, blocks):
                    update_block(s, block)

            if last:
                plain()
            else:
                pl.when(pcol > s + 1)(plain)

                @pl.when(pcol == s + 1)
                def _():
                    produce(s + 1, 0, live(s + 1) * per_block, True)

                    @pl.when(prow == s + 1)
                    def _():
                        update_block(s, 0)

    for s in range(sections):
        for chunk in range(tiles):
            top_flows[s].finish(chunk)

        @pl.when(pcol > s)
        def _(s=s):
            for chunk in range(tiles):
                row_flows[s].finish(chunk)

        owner = s // CORES

        @pl.when(core != s % CORES)
        def _(s=s):
            pick_copy(s, 0, 0, partner).wait_send()

        @pl.when(both(core == s % CORES, x != owner))
        def _(s=s):
            pick_copy(s, 0, 1, partner).wait_send()

        for k in range(2):
            for way in range(4):

                @pl.when(sends[s][k][way][0])
                def _(s=s, k=k, way=way):
                    def body(i, carry):
                        col_copy(s, k, i, way).wait_send()
                        return carry

                    lax.fori_loop(0, live(s) * per_block, body, 0)


def on_device(matrix, pivots, lower_inv, upper_inv):
    prow_count = lax.axis_size("prow")
    pcol_count = lax.axis_size("pcol")
    tile = matrix[0, 0]
    rows, width = tile.shape
    sections = pivots.shape[0]
    blocks = rows // width
    assert width == pivots.shape[1] and sections <= prow_count and sections <= pcol_count
    tiles = 3
    relays = blocks * 6
    dma = pltpu.SemaphoreType.DMA
    out = pl.pallas_call(
        functools.partial(factor_kernel, prow_count, pcol_count, sections, width, blocks),
        out_shape=jax.ShapeDtypeStruct(tile.shape, tile.dtype),
        in_specs=[pl.BlockSpec(memory_space=pl.ANY)] * 4,
        out_specs=pl.BlockSpec(memory_space=pltpu.VMEM),
        scratch_shapes=[
            pltpu.VMEM((rows, width), F32),
            pltpu.VMEM(pivots.shape, jnp.int32),
            pltpu.VMEM((width, width), F32),
            pltpu.VMEM((width, width), F32),
            pltpu.VMEM((3, rows, width), BF16),
            pltpu.VMEM((sections * width, width), F32),
            pltpu.VMEM((3, sections * width, width), BF16),
            pltpu.VMEM((sections, width, width), F32),
            pltpu.VMEM((sections, 3, width, width), F32),
            pltpu.VMEM((sections, width, width), F32),
            pltpu.VMEM((sections, rows, width), F32),
            pltpu.VMEM((3 * width, width), BF16),
            pltpu.VMEM((width, 3 * width), BF16),
            pltpu.VMEM((3 * width, width), BF16),
            pltpu.VMEM((3 * width, width), BF16),
            dma((5,)),
            dma((sections, 3, tiles)),
            dma((sections, tiles)),
            dma((sections, 2)),
            dma((sections, 3)),
            dma((sections, 3, tiles)),
            dma((sections, tiles)),
            dma((sections, 2, 4, relays)),
            dma((sections, 2, relays)),
        ],
        compiler_params=pltpu.CompilerParams(
            collective_id=0, has_side_effects=True, vmem_limit_bytes=60 * 1024 * 1024
        ),
    )(tile, pivots, lower_inv, upper_inv)
    return out[None, None]


def solution(mesh):
    return jax.shard_map(
        on_device,
        mesh=mesh,
        in_specs=(P("prow", "pcol", None, None), P(), P(), P()),
        out_specs=P("prow", "pcol", None, None),
        check_vma=False,
    )
```

```python
import functools

import jax
import jax.numpy as jnp
from jax import lax
from jax.experimental import pallas as pl
from jax.experimental.pallas import tpu as pltpu
from jax.sharding import PartitionSpec as P

MESH = pl.DeviceIdType.MESH
CORES = 2
F32 = jnp.float32
BF16 = jnp.bfloat16
HOP = 3
EARLY = 4
LAG = 2


def grid_width(count):
    width = 1
    while (2 * width) * (2 * width) <= count:
        width *= 2
    return width if count % width == 0 else 1


def both(*conds):
    out = conds[0]
    for cond in conds[1:]:
        out = jnp.logical_and(out, cond)
    return out


def entry_barrier(neighbours):
    barrier = pltpu.get_barrier_semaphore()
    total = jnp.int32(0)
    for cond, device in neighbours:
        total = total + jnp.where(cond, 1, 0).astype(jnp.int32)

        @pl.when(cond)
        def _(device=device):
            pl.semaphore_signal(barrier, inc=1, device_id=device, device_id_type=MESH)

    pl.semaphore_wait(barrier, total)


def line_ways(prow, prow_count):
    x, core = prow // CORES, prow % CORES
    chips = prow_count // CORES
    return [
        (x + 1 < chips, {"prow": prow + CORES}),
        (x > 0, {"prow": prow - CORES}),
        (prow >= 0, {"prow": x * CORES + (CORES - 1 - core)}),
    ]


def line_sends(prow, prow_count, source):
    x, core = prow // CORES, prow % CORES
    ways = line_ways(prow, prow_count)
    sx, sc = source // CORES, source % CORES
    return [
        (both(ways[0][0], core == sc, x >= sx), ways[0][1]),
        (both(ways[1][0], core == sc, x <= sx), ways[1][1]),
        (core == sc, ways[2][1]),
    ]


def grid_ways(pcol, pcol_count):
    width = grid_width(pcol_count)
    height = pcol_count // width
    z, y = pcol // width, pcol % width
    return [
        (z + 1 < height, {"pcol": pcol + width}),
        (z > 0, {"pcol": pcol - width}),
        (y + 1 < width, {"pcol": pcol + 1}),
        (y > 0, {"pcol": pcol - 1}),
    ]


def tree_plan(pcol_count, source, first_axis):
    width = grid_width(pcol_count)
    extent = (pcol_count // width, width)
    src = (source // width, source % width)
    a, b = first_axis, 1 - first_axis
    near = src[a] + 1 if src[a] + 1 < extent[a] else src[a] - 1

    def toward(at, goal):
        return at + (goal > at) - (goal < at)

    parent = {}
    for node in range(pcol_count):
        pos = [node // width, node % width]
        if node == source:
            continue
        if pos[b] == src[b]:
            pos[a] = toward(pos[a], src[a])
        elif pos[a] != src[a] or extent[a] == 1:
            pos[b] = toward(pos[b], src[b])
        else:
            pos[a] = near
        parent[node] = pos[0] * width + pos[1]
    hops, used = {source: 0}, set()
    for node in range(pcol_count):
        path = [node]
        while path[-1] != source:
            path.append(parent[path[-1]])
        hops[node] = len(path) - 1
        if node > source:
            used.update(path)
    steps = (width, -width, 1, -1)
    senders = [
        [parent[c] for c in used if c != source and c - parent[c] == step]
        if step not in steps[:way] else []
        for way, step in enumerate(steps)
    ]
    return hops, used - {source}, senders


def pick_static(index, table):
    out = jnp.int32(0)
    for key, value in table.items():
        out = jnp.where(index == key, value, out)
    return out


def among(index, members):
    mask = sum(1 << member for member in set(members))
    return (lax.shift_right_logical(jnp.int32(mask), index) & 1) == 1


class Flow:
    def __init__(self, mine, start_ref, land_ref, sends, send_sem, recv_sem, rows):
        self.mine, self.start_ref, self.land_ref = mine, start_ref, land_ref
        self.sends, self.send_sem, self.recv_sem, self.rows = sends, send_sem, recv_sem, rows

    def copy(self, chunk, way, ref):
        piece = pl.ds(chunk * self.rows, self.rows)
        return pltpu.make_async_remote_copy(
            src_ref=ref.at[piece],
            dst_ref=self.land_ref.at[piece],
            send_sem=self.send_sem.at[way, chunk],
            recv_sem=self.recv_sem.at[chunk],
            device_id=self.sends[way][1],
            device_id_type=MESH,
        )

    def send(self, chunk, ref):
        for way, (cond, _device) in enumerate(self.sends):

            @pl.when(cond)
            def _(way=way):
                self.copy(chunk, way, ref).start()

    def pass_on(self, chunk):
        @pl.when(jnp.logical_not(self.mine))
        def _():
            self.copy(chunk, 0, self.land_ref).wait_recv()
            self.send(chunk, self.land_ref)

    def finish(self, chunk):
        for way, (cond, _device) in enumerate(self.sends):

            @pl.when(cond)
            def _(way=way):
                self.copy(chunk, way, self.land_ref).wait_send()


def split2(value):
    high = value.astype(BF16)
    low = (value - high.astype(F32)).astype(BF16)
    return high, low


def split3(value):
    high = value.astype(BF16)
    rest = value - high.astype(F32)
    middle = rest.astype(BF16)
    low = (rest - middle.astype(F32)).astype(BF16)
    return high, middle, low


def wide(value):
    high, low = split2(value)
    return jnp.concatenate([high, high, low], axis=1)


def dot(left, right):
    return jnp.dot(left, right, preferred_element_type=F32)


def factor_kernel(
    prow_count, pcol_count, sections, width, blocks,
    tile_ref, pivots_ref, lower_ref, upper_ref, final_ref,
    out_ref, first, pivot, low_in, up_in, parts, top, top_parts, picked, picked_in,
    row_panel, col_panel, row_stack, low_wide, up_stack, core_stack,
    local_sem, top_send, top_recv, pick_send, pick_recv,
    row_send, row_recv, col_send, col_recv,
):
    prow = lax.axis_index("prow")
    pcol = lax.axis_index("pcol")
    x, core = prow // CORES, prow % CORES
    chips = prow_count // CORES
    step_rows = width // 3
    tiles = width // step_rows
    relay_rows = col_panel.shape[1] // (2 * col_recv.shape[2])
    span = 2 * relay_rows
    per_block = width // span

    load_tile = pltpu.make_async_copy(tile_ref, first, local_sem.at[0])
    load_pivots = pltpu.make_async_copy(pivots_ref, pivot, local_sem.at[1])
    load_pivots.start()
    load_tile.start()
    owns_row = prow < sections
    owns_col = pcol < sections

    @pl.when(owns_row)
    def _():
        pltpu.make_async_copy(lower_ref.at[prow], low_in, local_sem.at[2]).start()

    @pl.when(owns_col)
    def _():
        pltpu.make_async_copy(upper_ref.at[pcol], up_in, local_sem.at[3]).start()

    top_flows = [
        Flow(
            prow == s, tile_ref, top.at[pl.ds(s * width, width)],
            line_sends(prow, prow_count, s), top_send.at[s], top_recv.at[s], step_rows,
        )
        for s in range(sections)
    ]
    row_flows = [
        Flow(
            prow == s, row_panel.at[s], row_panel.at[s],
            line_sends(prow, prow_count, s), row_send.at[s], row_recv.at[s], step_rows,
        )
        for s in range(sections)
    ]

    entry_barrier(line_ways(prow, prow_count) + grid_ways(pcol, pcol_count))

    for s in range(sections):

        @pl.when(prow == s)
        def _(s=s):
            for chunk in range(tiles):
                top_flows[s].send(chunk, tile_ref)
            pltpu.make_async_copy(
                tile_ref.at[pl.ds(0, width)], top.at[pl.ds(s * width, width)], local_sem.at[4]
            ).start()

    def lanes(count):
        return lax.broadcasted_iota(jnp.int32, (1, count), 1).astype(F32)

    def column(start):
        ids = lax.broadcasted_iota(jnp.int32, (step_rows, 1), 0)
        return (ids + start).astype(F32)

    def pivot_row(s):
        return pivot[pl.ds(s, 1), :].astype(F32)

    def undo(rows, upto):
        for s in reversed(range(upto)):
            listed = pivot_row(s)
            shift = lanes(width) + F32(s * width) - listed
            moved = jnp.where(rows == listed, shift, F32(0))
            rows = rows + jnp.sum(moved, axis=1, keepdims=True)
        return rows

    def one_hot(rows, ids):
        return jnp.where(rows == ids, F32(1), F32(0)).astype(BF16)

    load_pivots.wait()
    load_tile.wait()

    def cut_tile(i, carry):
        at = pl.ds(pl.multiple_of(i * step_rows, step_rows), step_rows)
        for k, part in enumerate(split3(first[at, :])):
            parts[k, at, :] = part
        return carry

    lax.fori_loop(0, tiles * blocks, cut_tile, 0)

    def pick_copy(s, slot, where, device):
        return pltpu.make_async_remote_copy(
            src_ref=picked.at[s],
            dst_ref=picked_in.at[s, slot],
            send_sem=pick_send.at[s, where],
            recv_sem=pick_recv.at[s, slot],
            device_id=device,
            device_id_type=MESH,
        )

    partner = {"prow": x * CORES + (CORES - 1 - core)}
    held_ids = jnp.concatenate(
        [
            lanes(width) + ((block * prow_count + prow) * width).astype(F32)
            for block in range(blocks)
        ],
        axis=1,
    )
    def pick_rows(s):
        def pick(i, carry):
            start = i * step_rows
            at = pl.ds(pl.multiple_of(start, step_rows), step_rows)
            rows = jnp.sum(
                jnp.where(column(start) == lanes(width), pivot_row(s), F32(0)),
                axis=1, keepdims=True,
            )
            chosen = one_hot(undo(rows, s), held_ids)
            picked[s, at, :] = (
                dot(chosen, parts[2]) + dot(chosen, parts[1]) + dot(chosen, parts[0])
            )
            return carry

        lax.fori_loop(0, tiles, pick, 0)

        @pl.when(core != s % CORES)
        def _():
            pick_copy(s, 0, 0, partner).start()

    def add_in(s, slot):
        pick_copy(s, slot, 1, partner).wait_recv()

        def add(i, carry):
            at = pl.ds(pl.multiple_of(i * step_rows, step_rows), step_rows)
            picked[s, at, :] += picked_in[s, slot, at, :]
            return carry

        lax.fori_loop(0, tiles, add, 0)

    def pass_picked(s, when):
        owner = s // CORES

        @pl.when(both(core == s % CORES, x != owner, when))
        def _():
            add_in(s, 0)

            @pl.when(both(x < owner, x > 0))
            def _():
                add_in(s, 1)

            @pl.when(both(x > owner, x < chips - 1))
            def _():
                add_in(s, 2)

            @pl.when(x < owner)
            def _():
                pick_copy(s, 1, 1, {"prow": prow + CORES}).start()

            @pl.when(x > owner)
            def _():
                pick_copy(s, 2, 1, {"prow": prow - CORES}).start()

    def urgent(s):
        return pcol > 0 if s == 0 else both(pcol >= 0, s >= CORES) | (pcol == 0)

    pick_rows(0)
    for s in range(1, sections):
        pick_rows(s)
        pass_picked(s - 1, urgent(s - 1))
    pass_picked(sections - 1, urgent(sections - 1))

    @pl.when(owns_row)
    def _():
        pltpu.make_async_copy(lower_ref.at[prow], low_in, local_sem.at[2]).wait()

        def prepare(i, carry):
            start = i * step_rows
            at = pl.ds(pl.multiple_of(start, step_rows), step_rows)
            below = column(start) > lanes(width)
            same = column(start) == lanes(width)
            unit = jnp.where(below, low_in[at, :], jnp.where(same, F32(1), F32(0)))
            low_wide[at, :] = wide(unit)
            return carry

        lax.fori_loop(0, tiles, prepare, 0)

    def stack(ref, i, value):
        high, low = split2(value)
        start = i * step_rows
        for k, part in enumerate((high, low, high)):
            at = pl.ds(pl.multiple_of(k * width + start, step_rows), step_rows)
            ref[at, :] = part

    @pl.when(owns_col)
    def _():
        pltpu.make_async_copy(upper_ref.at[pcol], up_in, local_sem.at[3]).wait()

        def prepare(i, carry):
            start = i * step_rows
            at = pl.ds(pl.multiple_of(start, step_rows), step_rows)
            kept = jnp.where(column(start) <= lanes(width), up_in[at, :], F32(0))
            stack(up_stack, i, kept)
            return carry

        lax.fori_loop(0, tiles, prepare, 0)

    for chunk in range(tiles):
        for flow in top_flows:
            flow.pass_on(chunk)
    for s in range(sections):

        @pl.when(prow == s)
        def _(s=s):
            pltpu.make_async_copy(
                tile_ref.at[pl.ds(0, width)], top.at[pl.ds(s * width, width)], local_sem.at[4]
            ).wait()

    def take_picked(s):
        owner = s // CORES
        add_in(s, 0)
        if owner > 0:
            add_in(s, 1)
        if owner < chips - 1:
            add_in(s, 2)
        out_ref[pl.ds(0, width), :] = picked[s]

    def row_product(s):
        def cut(i, carry):
            at = pl.ds(pl.multiple_of(i * step_rows, step_rows), step_rows)
            stack(core_stack, i, out_ref[at, :])
            return carry

        lax.fori_loop(0, tiles, cut, 0)
        for chunk in range(tiles):
            at = pl.ds(chunk * step_rows, step_rows)
            value = dot(low_wide[at, :], core_stack[...])
            row_panel[s, at, :] = value
            out_ref[at, :] = value
            if chunk > 0:
                row_flows[s].send(chunk - 1, row_panel.at[s])
        row_flows[s].send(tiles - 1, row_panel.at[s])

    @pl.when(both(prow == 0, pcol > 0))
    def _():
        take_picked(0)
        row_product(0)

    for s in range(sections):
        pass_picked(s, jnp.logical_not(urgent(s)))

    def cut_top(i, carry):
        at = pl.ds(pl.multiple_of(i * step_rows, step_rows), step_rows)
        for k, part in enumerate(split3(top[at, :])):
            top_parts[k, at, :] = part
        return carry

    lax.fori_loop(0, tiles * sections, cut_top, 0)

    def settle(block):
        def place(i, carry):
            start = i * step_rows
            at = pl.ds(pl.multiple_of(block * width + start, step_rows), step_rows)
            rows = column(start + (block * prow_count + prow) * width)
            rows = undo(rows, sections)
            chosen = one_hot(rows, lanes(sections * width))
            value = (
                dot(chosen, top_parts[2]) + dot(chosen, top_parts[1]) + dot(chosen, top_parts[0])
            )
            out_ref[at, :] = jnp.where(rows < F32(sections * width), value, first[at, :])
            return carry

        lax.fori_loop(0, tiles, place, 0)

    ways = grid_ways(pcol, pcol_count)
    plans = [[tree_plan(pcol_count, s, k) for k in range(2)] for s in range(sections)]
    sends = [[[among(pcol, who) for who in plan[2]] for plan in pair] for pair in plans]
    gets = [[among(pcol, plan[1]) for plan in pair] for pair in plans]

    def farthest(s, node):
        return max(plan[0][node] for plan in plans[s])

    def live(s):
        return jnp.where(prow > s, blocks, blocks - 1)

    def place_of(s, i):
        turn = lax.div(i, per_block)
        block = blocks - live(s) + turn
        return block * width + (i - turn * per_block) * span

    def col_copy(s, k, i, way):
        start = pl.multiple_of(place_of(s, i) + k * relay_rows, relay_rows)
        piece = pl.ds(start, relay_rows)
        return pltpu.make_async_remote_copy(
            src_ref=col_panel.at[s, piece],
            dst_ref=col_panel.at[s, piece],
            send_sem=col_send.at[s, k, way],
            recv_sem=col_recv.at[s, k, i],
            device_id=ways[way][1],
            device_id_type=MESH,
        )

    def col_start(s, k, i):
        for way in range(4):

            @pl.when(sends[s][k][way])
            def _(way=way):
                col_copy(s, k, i, way).start()

    def update(s, at):
        return out_ref[at, :] - dot(wide(col_panel[s, at, :]), row_stack[s])

    def rows_of(s, i):
        return pl.ds(pl.multiple_of(place_of(s, i), span), span)

    def produce(s, i, value):
        at = rows_of(s, i)
        value = dot(wide(value), up_stack[...])
        col_panel[s, at, :] = value
        out_ref[at, :] = value

    def start_both(s, i):
        for k in range(2):
            col_start(s, k, i)

    def produce_first(start, stop):
        def body(i, carry):
            produce(0, i, out_ref[rows_of(0, i), :])

            @pl.when(i > start)
            def _():
                start_both(0, i - 1)

            return carry

        lax.fori_loop(start, stop, body, 0)
        start_both(0, stop - 1)

    def forwards(s):
        return both(core == s % CORES, prow != s)

    def pass_row(s):
        for chunk in range(tiles):
            row_flows[s].pass_on(chunk)

    def take_row(s):
        @pl.when(jnp.logical_not(forwards(s)))
        def _():
            pass_row(s)

        def cut(i, carry):
            at = pl.ds(pl.multiple_of(i * step_rows, step_rows), step_rows)
            stack(row_stack.at[s], i, row_panel[s, at, :])
            return carry

        lax.fori_loop(0, tiles, cut, 0)

    @pl.when(pcol == 0)
    def _():
        @pl.when(jnp.logical_not(owns_row))
        def _():
            settle(0)
            produce_first(0, per_block)

        for block in range(1, blocks):
            settle(block)
        for s in range(1, sections):

            @pl.when(prow == s)
            def _(s=s):
                take_picked(s)

        produce_first(jnp.where(owns_row, 0, per_block), live(0) * per_block)

    @pl.when(pcol > 0)
    def _():
        for block in range(1, blocks):
            settle(block)

        @pl.when(jnp.logical_not(owns_row))
        def _():
            settle(0)

    begin, begin_of, lates, computes, counts = jnp.int32(0), [], [], [], []
    forward_at = []
    for s in range(sections):
        counts.append(live(s) * per_block)
        begin_of.append(begin)
        lates.append(
            [begin + pick_static(pcol, {n: HOP * h for n, h in plan[0].items()}) for plan in plans[s]]
        )
        lag = {n: HOP * farthest(s, n) + (LAG if n != s + 1 else 0) for n in range(pcol_count)}
        early = {n: HOP * farthest(s, n) - EARLY for n in range(pcol_count)}
        forward_at.append(begin + pick_static(pcol, early))
        computes.append(begin + pick_static(pcol, lag))
        if s + 1 < sections:
            begin = begin + HOP * farthest(s, s + 1) + 1
            begin = begin + jnp.where(prow == s + 1, per_block, 0)
            for n in range(s + 2, pcol_count):
                ahead = HOP * (farthest(s, s + 1) + farthest(s + 1, n) - farthest(s, n))
                assert ahead + 1 >= (LAG if n == s + 2 else 0)

    def inline(s):
        return both(pcol > s, x == s // CORES) if s + 1 == sections else pcol > s

    def compute(s, j):
        last = s + 1 == sections
        skip = 0 if last else counts[s] - counts[s + 1]

        @pl.when(j == 0)
        def _():
            if s == 0:
                for other in range(1, sections):

                    @pl.when(prow == other)
                    def _(other=other):
                        take_picked(other)

            take_row(s)

        at = rows_of(s, j)
        value = update(s, at)
        if last:
            out_ref[at, :] = value
            return
        makes = both(pcol == s + 1, j >= skip)

        @pl.when(jnp.logical_not(makes))
        def _():
            out_ref[at, :] = value

        @pl.when(makes)
        def _():
            produce(s + 1, j - skip, value)

        @pl.when(both(prow == s + 1, pcol > s + 1, j == per_block - 1))
        def _():
            row_product(s + 1)

    def turn(t, carry):
        for s in range(sections):
            for k in range(2):
                i = t - lates[s][k]

                @pl.when(both(gets[s][k], i >= 0, i < counts[s]))
                def _(s=s, k=k, i=i):
                    col_copy(s, k, i, 0).wait_recv()
                    col_start(s, k, i)

            @pl.when(both(inline(s), forwards(s), t == jnp.maximum(forward_at[s], 0)))
            def _(s=s):
                pass_row(s)

            if s > 0:
                i = t - begin_of[s]

                @pl.when(both(pcol == s, i >= 0, i < counts[s]))
                def _(s=s, i=i):
                    start_both(s, i)

            j = t - computes[s]

            @pl.when(both(inline(s), j >= 0, j < counts[s]))
            def _(s=s, j=j):
                compute(s, j)

        return carry

    stop = jnp.int32(0)
    for s in range(sections):
        stop = jnp.maximum(stop, jnp.where(inline(s), computes[s] + counts[s], 0))
        for k in range(2):
            stop = jnp.maximum(stop, jnp.where(gets[s][k], lates[s][k] + counts[s], 0))
        if s > 0:
            stop = jnp.maximum(stop, jnp.where(pcol == s, begin_of[s] + counts[s], 0))
    lax.fori_loop(0, stop, turn, 0)
    last = sections - 1

    @pl.when(both(pcol > last, jnp.logical_not(inline(last))))
    def _():
        @pl.when(forwards(last))
        def _():
            pass_row(last)

        take_row(last)

        def body(i, carry):
            at = pl.ds(pl.multiple_of(i * step_rows, step_rows), step_rows)
            out_ref[at, :] = update(last, at)
            return carry

        lax.fori_loop((blocks - live(last)) * tiles, blocks * tiles, body, 0)

    @pl.when(both(prow == 0, pcol == 0))
    def _():
        take_picked(0)

    save = pltpu.make_async_copy(out_ref, final_ref, local_sem.at[0])
    save.start()
    for s in range(sections):
        for chunk in range(tiles):
            top_flows[s].finish(chunk)

        @pl.when(pcol > s)
        def _(s=s):
            for chunk in range(tiles):
                row_flows[s].finish(chunk)

        owner = s // CORES

        @pl.when(core != s % CORES)
        def _(s=s):
            pick_copy(s, 0, 0, partner).wait_send()

        @pl.when(both(core == s % CORES, x != owner))
        def _(s=s):
            pick_copy(s, 0, 1, partner).wait_send()

        for k in range(2):
            for way in range(4):
                for count in (blocks - 1, blocks):

                    @pl.when(both(sends[s][k][way], live(s) == count))
                    def _(s=s, k=k, way=way, count=count):
                        piece = pl.ds(0, count * width // 2)
                        pltpu.make_async_remote_copy(
                            src_ref=col_panel.at[s, piece],
                            dst_ref=col_panel.at[s, piece],
                            send_sem=col_send.at[s, k, way],
                            recv_sem=col_recv.at[s, k, 0],
                            device_id=ways[way][1],
                            device_id_type=MESH,
                        ).wait_send()

    save.wait()


def on_device(matrix, pivots, lower_inv, upper_inv):
    prow_count = lax.axis_size("prow")
    pcol_count = lax.axis_size("pcol")
    tile = matrix[0, 0]
    rows, width = tile.shape
    sections = pivots.shape[0]
    blocks = rows // width
    assert width == pivots.shape[1] and sections <= prow_count and sections <= pcol_count
    tiles = 3
    relays = blocks * 6
    dma = pltpu.SemaphoreType.DMA
    out = pl.pallas_call(
        functools.partial(factor_kernel, prow_count, pcol_count, sections, width, blocks),
        out_shape=jax.ShapeDtypeStruct(tile.shape, tile.dtype),
        in_specs=[pl.BlockSpec(memory_space=pl.ANY)] * 4,
        out_specs=pl.BlockSpec(memory_space=pl.ANY),
        scratch_shapes=[
            pltpu.VMEM((rows, width), F32),
            pltpu.VMEM((rows, width), F32),
            pltpu.VMEM(pivots.shape, jnp.int32),
            pltpu.VMEM((width, width), F32),
            pltpu.VMEM((width, width), F32),
            pltpu.VMEM((3, rows, width), BF16),
            pltpu.VMEM((sections * width, width), F32),
            pltpu.VMEM((3, sections * width, width), BF16),
            pltpu.VMEM((sections, width, width), F32),
            pltpu.VMEM((sections, 3, width, width), F32),
            pltpu.VMEM((sections, width, width), F32),
            pltpu.VMEM((sections, rows, width), F32),
            pltpu.VMEM((sections, 3 * width, width), BF16),
            pltpu.VMEM((width, 3 * width), BF16),
            pltpu.VMEM((3 * width, width), BF16),
            pltpu.VMEM((3 * width, width), BF16),
            dma((5,)),
            dma((sections, 3, tiles)),
            dma((sections, tiles)),
            dma((sections, 2)),
            dma((sections, 3)),
            dma((sections, 3, tiles)),
            dma((sections, tiles)),
            dma((sections, 2, 4)),
            dma((sections, 2, relays)),
        ],
        compiler_params=pltpu.CompilerParams(
            collective_id=0, has_side_effects=True, vmem_limit_bytes=60 * 1024 * 1024
        ),
    )(tile, pivots, lower_inv, upper_inv)
    return out[None, None]


def solution(mesh):
    return jax.shard_map(
        on_device,
        mesh=mesh,
        in_specs=(P("prow", "pcol", None, None), P(), P(), P()),
        out_specs=P("prow", "pcol", None, None),
        check_vma=False,
    )
```

```python
import functools

import jax
import jax.numpy as jnp
from jax import lax
from jax.experimental import pallas as pl
from jax.experimental.pallas import tpu as pltpu
from jax.sharding import PartitionSpec as P

MESH = pl.DeviceIdType.MESH
CORES = 2
F32 = jnp.float32
BF16 = jnp.bfloat16
HOP = 3
EARLY = (4, 0)
PICK = 384
LAG = 2


def grid_width(count):
    width = 1
    while (2 * width) * (2 * width) <= count:
        width *= 2
    return width if count % width == 0 else 1


def both(*conds):
    out = conds[0]
    for cond in conds[1:]:
        out = jnp.logical_and(out, cond)
    return out


def entry_barrier(neighbours):
    barrier = pltpu.get_barrier_semaphore()
    total = jnp.int32(0)
    for cond, device in neighbours:
        total = total + jnp.where(cond, 1, 0).astype(jnp.int32)

        @pl.when(cond)
        def _(device=device):
            pl.semaphore_signal(barrier, inc=1, device_id=device, device_id_type=MESH)

    pl.semaphore_wait(barrier, total)


def line_ways(prow, prow_count):
    x, core = prow // CORES, prow % CORES
    chips = prow_count // CORES
    return [
        (x + 1 < chips, {"prow": prow + CORES}),
        (x > 0, {"prow": prow - CORES}),
        (prow >= 0, {"prow": x * CORES + (CORES - 1 - core)}),
    ]


def line_sends(prow, prow_count, source):
    x, core = prow // CORES, prow % CORES
    ways = line_ways(prow, prow_count)
    sx, sc = source // CORES, source % CORES
    return [
        (both(ways[0][0], core == sc, x >= sx), ways[0][1]),
        (both(ways[1][0], core == sc, x <= sx), ways[1][1]),
        (core == sc, ways[2][1]),
    ]


def grid_ways(pcol, pcol_count):
    width = grid_width(pcol_count)
    height = pcol_count // width
    z, y = pcol // width, pcol % width
    return [
        (z + 1 < height, {"pcol": pcol + width}),
        (z > 0, {"pcol": pcol - width}),
        (y + 1 < width, {"pcol": pcol + 1}),
        (y > 0, {"pcol": pcol - 1}),
    ]


def tree_plan(pcol_count, source, first_axis):
    width = grid_width(pcol_count)
    extent = (pcol_count // width, width)
    src = (source // width, source % width)
    a, b = first_axis, 1 - first_axis
    near = src[a] + 1 if src[a] + 1 < extent[a] else src[a] - 1

    def toward(at, goal):
        return at + (goal > at) - (goal < at)

    parent = {}
    for node in range(pcol_count):
        pos = [node // width, node % width]
        if node == source:
            continue
        if pos[b] == src[b]:
            pos[a] = toward(pos[a], src[a])
        elif pos[a] != src[a] or extent[a] == 1:
            pos[b] = toward(pos[b], src[b])
        else:
            pos[a] = near
        parent[node] = pos[0] * width + pos[1]
    hops, used = {source: 0}, set()
    for node in range(pcol_count):
        path = [node]
        while path[-1] != source:
            path.append(parent[path[-1]])
        hops[node] = len(path) - 1
        if node > source:
            used.update(path)
    steps = (width, -width, 1, -1)
    senders = [
        [parent[c] for c in used if c != source and c - parent[c] == step]
        if step not in steps[:way] else []
        for way, step in enumerate(steps)
    ]
    return hops, used - {source}, senders


def pick_static(index, table):
    out = jnp.int32(0)
    for key, value in table.items():
        out = jnp.where(index == key, value, out)
    return out


def among(index, members):
    mask = sum(1 << member for member in set(members))
    return (lax.shift_right_logical(jnp.int32(mask), index) & 1) == 1


class Flow:
    def __init__(self, mine, start_ref, land_ref, sends, send_sem, recv_sem, rows):
        self.mine, self.start_ref, self.land_ref = mine, start_ref, land_ref
        self.sends, self.send_sem, self.recv_sem, self.rows = sends, send_sem, recv_sem, rows

    def copy(self, chunk, way, ref):
        piece = pl.ds(chunk * self.rows, self.rows)
        return pltpu.make_async_remote_copy(
            src_ref=ref.at[piece],
            dst_ref=self.land_ref.at[piece],
            send_sem=self.send_sem.at[way, chunk],
            recv_sem=self.recv_sem.at[chunk],
            device_id=self.sends[way][1],
            device_id_type=MESH,
        )

    def send(self, chunk, ref):
        for way, (cond, _device) in enumerate(self.sends):

            @pl.when(cond)
            def _(way=way):
                self.copy(chunk, way, ref).start()

    def pass_on(self, chunk):
        @pl.when(jnp.logical_not(self.mine))
        def _():
            self.copy(chunk, 0, self.land_ref).wait_recv()
            self.send(chunk, self.land_ref)

    def finish(self, chunk):
        for way, (cond, _device) in enumerate(self.sends):

            @pl.when(cond)
            def _(way=way):
                self.copy(chunk, way, self.land_ref).wait_send()


def split2(value):
    high = value.astype(BF16)
    low = (value - high.astype(F32)).astype(BF16)
    return high, low


def split3(value):
    high = value.astype(BF16)
    rest = value - high.astype(F32)
    middle = rest.astype(BF16)
    low = (rest - middle.astype(F32)).astype(BF16)
    return high, middle, low


def wide(value):
    high, low = split2(value)
    return jnp.concatenate([high, high, low], axis=1)


def dot(left, right):
    return jnp.dot(left, right, preferred_element_type=F32)


def factor_kernel(
    prow_count, pcol_count, sections, width, blocks,
    tile_ref, pivots_ref, lower_ref, upper_ref, final_ref,
    out_ref, first, pivot, low_in, up_in, parts, top, top_parts, picked, picked_in,
    row_panel, col_panel, row_stack, low_wide, up_stack, core_stack,
    local_sem, top_send, top_recv, pick_send, pick_recv,
    row_send, row_recv, col_send, col_recv,
):
    prow = lax.axis_index("prow")
    pcol = lax.axis_index("pcol")
    x, core = prow // CORES, prow % CORES
    chips = prow_count // CORES
    step_rows = width // 3
    tiles = width // step_rows
    relay_rows = col_panel.shape[1] // (2 * col_recv.shape[2])
    span = 2 * relay_rows
    per_block = width // span

    load_tile = pltpu.make_async_copy(tile_ref, first, local_sem.at[0])
    load_pivots = pltpu.make_async_copy(pivots_ref, pivot, local_sem.at[1])
    load_pivots.start()
    load_tile.start()
    owns_row = prow < sections
    owns_col = pcol < sections

    @pl.when(owns_row)
    def _():
        pltpu.make_async_copy(lower_ref.at[prow], low_in, local_sem.at[2]).start()

    @pl.when(owns_col)
    def _():
        pltpu.make_async_copy(upper_ref.at[pcol], up_in, local_sem.at[3]).start()

    top_flows = [
        Flow(
            prow == s, tile_ref, top.at[pl.ds(s * width, width)],
            line_sends(prow, prow_count, s), top_send.at[s], top_recv.at[s], step_rows,
        )
        for s in range(sections)
    ]
    row_flows = [
        Flow(
            prow == s, row_panel.at[s], row_panel.at[s],
            line_sends(prow, prow_count, s), row_send.at[s], row_recv.at[s], step_rows,
        )
        for s in range(sections)
    ]

    entry_barrier(line_ways(prow, prow_count) + grid_ways(pcol, pcol_count))

    for s in range(sections):

        @pl.when(prow == s)
        def _(s=s):
            for chunk in range(tiles):
                top_flows[s].send(chunk, tile_ref)
            pltpu.make_async_copy(
                tile_ref.at[pl.ds(0, width)], top.at[pl.ds(s * width, width)], local_sem.at[4]
            ).start()

    def lanes(count):
        return lax.broadcasted_iota(jnp.int32, (1, count), 1).astype(F32)

    def column(start, rows=step_rows):
        ids = lax.broadcasted_iota(jnp.int32, (rows, 1), 0)
        return (ids + start).astype(F32)

    def pivot_row(s):
        return pivot[pl.ds(s, 1), :].astype(F32)

    def undo(rows, upto):
        for s in reversed(range(upto)):
            listed = pivot_row(s)
            shift = lanes(width) + F32(s * width) - listed
            moved = jnp.where(rows == listed, shift, F32(0))
            rows = rows + jnp.sum(moved, axis=1, keepdims=True)
        return rows

    def one_hot(rows, ids):
        return jnp.where(rows == ids, F32(1), F32(0)).astype(BF16)

    load_pivots.wait()
    load_tile.wait()

    def cut_tile(i, carry):
        at = pl.ds(pl.multiple_of(i * step_rows, step_rows), step_rows)
        for k, part in enumerate(split3(first[at, :])):
            parts[k, at, :] = part
        return carry

    lax.fori_loop(0, tiles * blocks, cut_tile, 0)

    def pick_copy(s, slot, where, device):
        return pltpu.make_async_remote_copy(
            src_ref=picked.at[s],
            dst_ref=picked_in.at[s, slot],
            send_sem=pick_send.at[s, where],
            recv_sem=pick_recv.at[s, slot],
            device_id=device,
            device_id_type=MESH,
        )

    partner = {"prow": x * CORES + (CORES - 1 - core)}
    held_ids = jnp.concatenate(
        [
            lanes(width) + ((block * prow_count + prow) * width).astype(F32)
            for block in range(blocks)
        ],
        axis=1,
    )
    def pick_rows(s):
        def pick(i, carry):
            start = i * PICK
            at = pl.ds(pl.multiple_of(start, PICK), PICK)
            rows = jnp.sum(
                jnp.where(column(start, PICK) == lanes(width), pivot_row(s), F32(0)),
                axis=1, keepdims=True,
            )
            chosen = one_hot(undo(rows, s), held_ids)
            picked[s, at, :] = (
                dot(chosen, parts[2]) + dot(chosen, parts[1]) + dot(chosen, parts[0])
            )
            return carry

        lax.fori_loop(0, width // PICK, pick, 0)

        @pl.when(core != s % CORES)
        def _():
            pick_copy(s, 0, 0, partner).start()

    def add_in(s, slot):
        pick_copy(s, slot, 1, partner).wait_recv()

        def add(i, carry):
            at = pl.ds(pl.multiple_of(i * step_rows, step_rows), step_rows)
            picked[s, at, :] += picked_in[s, slot, at, :]
            return carry

        lax.fori_loop(0, tiles, add, 0)

    def pass_picked(s, when):
        owner = s // CORES

        @pl.when(both(core == s % CORES, x != owner, when))
        def _():
            add_in(s, 0)

            @pl.when(both(x < owner, x > 0))
            def _():
                add_in(s, 1)

            @pl.when(both(x > owner, x < chips - 1))
            def _():
                add_in(s, 2)

            @pl.when(x < owner)
            def _():
                pick_copy(s, 1, 1, {"prow": prow + CORES}).start()

            @pl.when(x > owner)
            def _():
                pick_copy(s, 2, 1, {"prow": prow - CORES}).start()

    def urgent(s):
        return pcol > 0 if s == 0 else both(pcol >= 0, s >= CORES) | (pcol == 0)

    def pick_all(order):
        for s in order:
            pick_rows(s)
            pass_picked(s, urgent(s))

    @pl.when(pcol == 0)
    def _():
        pick_all([*range(1, sections), 0])

    @pl.when(pcol > 0)
    def _():
        pick_all([*range(sections)])


    @pl.when(owns_row)
    def _():
        pltpu.make_async_copy(lower_ref.at[prow], low_in, local_sem.at[2]).wait()

        def prepare(i, carry):
            start = i * step_rows
            at = pl.ds(pl.multiple_of(start, step_rows), step_rows)
            below = column(start) > lanes(width)
            same = column(start) == lanes(width)
            unit = jnp.where(below, low_in[at, :], jnp.where(same, F32(1), F32(0)))
            low_wide[at, :] = wide(unit)
            return carry

        lax.fori_loop(0, tiles, prepare, 0)

    def stack(ref, i, value):
        high, low = split2(value)
        start = i * step_rows
        for k, part in enumerate((high, low, high)):
            at = pl.ds(pl.multiple_of(k * width + start, step_rows), step_rows)
            ref[at, :] = part

    @pl.when(owns_col)
    def _():
        pltpu.make_async_copy(upper_ref.at[pcol], up_in, local_sem.at[3]).wait()

        def prepare(i, carry):
            start = i * step_rows
            at = pl.ds(pl.multiple_of(start, step_rows), step_rows)
            kept = jnp.where(column(start) <= lanes(width), up_in[at, :], F32(0))
            stack(up_stack, i, kept)
            return carry

        lax.fori_loop(0, tiles, prepare, 0)

    def take_picked(s):
        owner = s // CORES
        add_in(s, 0)
        if owner > 0:
            add_in(s, 1)
        if owner < chips - 1:
            add_in(s, 2)
        out_ref[pl.ds(0, width), :] = picked[s]

    ways = grid_ways(pcol, pcol_count)
    plans = [[tree_plan(pcol_count, s, k) for k in range(2)] for s in range(sections)]
    sends = [[[among(pcol, who) for who in plan[2]] for plan in pair] for pair in plans]
    gets = [[among(pcol, plan[1]) for plan in pair] for pair in plans]

    def farthest(s, node):
        return max(plan[0][node] for plan in plans[s])

    def live(s):
        return jnp.where(prow > s, blocks, blocks - 1)

    def place_of(s, i):
        turn = lax.div(i, per_block)
        block = blocks - live(s) + turn
        return block * width + (i - turn * per_block) * span

    def col_copy(s, k, i, way):
        start = pl.multiple_of(place_of(s, i) + k * relay_rows, relay_rows)
        piece = pl.ds(start, relay_rows)
        return pltpu.make_async_remote_copy(
            src_ref=col_panel.at[s, piece],
            dst_ref=col_panel.at[s, piece],
            send_sem=col_send.at[s, k, way],
            recv_sem=col_recv.at[s, k, i],
            device_id=ways[way][1],
            device_id_type=MESH,
        )

    def col_start(s, k, i):
        for way in range(4):

            @pl.when(sends[s][k][way])
            def _(way=way):
                col_copy(s, k, i, way).start()

    def update(s, at):
        return out_ref[at, :] - dot(wide(col_panel[s, at, :]), row_stack[s])

    def rows_of(s, i):
        return pl.ds(pl.multiple_of(place_of(s, i), span), span)

    def produce(s, i, value):
        at = rows_of(s, i)
        value = dot(wide(value), up_stack[...])
        col_panel[s, at, :] = value
        out_ref[at, :] = value

    def start_both(s, i):
        for k in range(2):
            col_start(s, k, i)

    def produce_first(start, stop):
        def body(i, carry):
            produce(0, i, out_ref[rows_of(0, i), :])

            @pl.when(i > start)
            def _():
                start_both(0, i - 1)

            return carry

        lax.fori_loop(start, stop, body, 0)
        start_both(0, stop - 1)

    for s in range(1, min(CORES, sections)):

        @pl.when(both(pcol == 0, prow == s))
        def _(s=s):
            take_picked(s)
            produce_first(0, per_block)

    for chunk in range(tiles):
        for flow in top_flows:
            flow.pass_on(chunk)
    for s in range(sections):

        @pl.when(prow == s)
        def _(s=s):
            pltpu.make_async_copy(
                tile_ref.at[pl.ds(0, width)], top.at[pl.ds(s * width, width)], local_sem.at[4]
            ).wait()

    def row_product(s):
        def cut(i, carry):
            at = pl.ds(pl.multiple_of(i * step_rows, step_rows), step_rows)
            stack(core_stack, i, out_ref[at, :])
            return carry

        lax.fori_loop(0, tiles, cut, 0)
        for chunk in range(tiles):
            at = pl.ds(chunk * step_rows, step_rows)
            value = dot(low_wide[at, :], core_stack[...])
            row_panel[s, at, :] = value
            out_ref[at, :] = value
            if chunk > 0:
                row_flows[s].send(chunk - 1, row_panel.at[s])
        row_flows[s].send(tiles - 1, row_panel.at[s])

    @pl.when(both(prow == 0, pcol > 0))
    def _():
        take_picked(0)
        row_product(0)

    for s in range(sections):
        pass_picked(s, jnp.logical_not(urgent(s)))

    def cut_top(i, carry):
        at = pl.ds(pl.multiple_of(i * step_rows, step_rows), step_rows)
        for k, part in enumerate(split3(top[at, :])):
            top_parts[k, at, :] = part
        return carry

    lax.fori_loop(0, tiles * sections, cut_top, 0)

    def settle(block):
        def place(i, carry):
            start = i * PICK
            at = pl.ds(pl.multiple_of(block * width + start, PICK), PICK)
            rows = column(start + (block * prow_count + prow) * width, PICK)
            rows = undo(rows, sections)
            chosen = one_hot(rows, lanes(sections * width))
            value = (
                dot(chosen, top_parts[2]) + dot(chosen, top_parts[1]) + dot(chosen, top_parts[0])
            )
            out_ref[at, :] = jnp.where(rows < F32(sections * width), value, first[at, :])
            return carry

        lax.fori_loop(0, width // PICK, place, 0)

    def forwards(s):
        return both(core == s % CORES, prow != s)

    def pass_row(s):
        for chunk in range(tiles):
            row_flows[s].pass_on(chunk)

    def take_row(s):
        @pl.when(jnp.logical_not(forwards(s)))
        def _():
            pass_row(s)

        def cut(i, carry):
            at = pl.ds(pl.multiple_of(i * step_rows, step_rows), step_rows)
            stack(row_stack.at[s], i, row_panel[s, at, :])
            return carry

        lax.fori_loop(0, tiles, cut, 0)

    @pl.when(pcol == 0)
    def _():
        @pl.when(jnp.logical_not(owns_row))
        def _():
            settle(0)
            produce_first(0, per_block)

        for block in range(1, blocks):
            settle(block)
        for s in range(sections):
            if s == 0 or s >= CORES:

                @pl.when(prow == s)
                def _(s=s):
                    take_picked(s)

        done = jnp.logical_or(both(prow > 0, prow < CORES), jnp.logical_not(owns_row))
        produce_first(jnp.where(done, per_block, 0), live(0) * per_block)

    @pl.when(pcol > 0)
    def _():
        for block in range(1, blocks):
            settle(block)

        @pl.when(jnp.logical_not(owns_row))
        def _():
            settle(0)

    begin, begin_of, lates, computes, counts = jnp.int32(0), [], [], [], []
    forward_at = []
    for s in range(sections):
        counts.append(live(s) * per_block)
        begin_of.append(begin)
        lates.append(
            [begin + pick_static(pcol, {n: HOP * h for n, h in plan[0].items()}) for plan in plans[s]]
        )
        lag = {n: HOP * farthest(s, n) + (LAG if n != s + 1 else 0) for n in range(pcol_count)}
        early = {n: HOP * farthest(s, n) - EARLY[min(s, 1)] for n in range(pcol_count)}
        forward_at.append(begin + pick_static(pcol, early))
        computes.append(begin + pick_static(pcol, lag))
        if s + 1 < sections:
            begin = begin + HOP * farthest(s, s + 1) + 1
            begin = begin + jnp.where(prow == s + 1, per_block, 0)
            for n in range(s + 2, pcol_count):
                ahead = HOP * (farthest(s, s + 1) + farthest(s + 1, n) - farthest(s, n))
                assert ahead + 1 >= (LAG if n == s + 2 else 0)

    def inline(s):
        return pcol < 0 if s + 1 == sections else pcol > s

    def compute(s, j):
        last = s + 1 == sections
        skip = 0 if last else counts[s] - counts[s + 1]

        @pl.when(j == 0)
        def _():
            if s == 0:
                for other in range(1, sections):

                    @pl.when(prow == other)
                    def _(other=other):
                        take_picked(other)

            take_row(s)

        at = rows_of(s, j)
        value = update(s, at)
        if last:
            out_ref[at, :] = value
            return
        makes = both(pcol == s + 1, j >= skip)

        @pl.when(jnp.logical_not(makes))
        def _():
            out_ref[at, :] = value

        @pl.when(makes)
        def _():
            produce(s + 1, j - skip, value)

        @pl.when(both(prow == s + 1, pcol > s + 1, j == per_block - 1))
        def _():
            row_product(s + 1)

    def turn(t, carry):
        for s in range(sections):
            for k in range(2):
                i = t - lates[s][k]

                @pl.when(both(gets[s][k], i >= 0, i < counts[s]))
                def _(s=s, k=k, i=i):
                    col_copy(s, k, i, 0).wait_recv()
                    col_start(s, k, i)

            @pl.when(both(inline(s), forwards(s), t == jnp.maximum(forward_at[s], 0)))
            def _(s=s):
                pass_row(s)

            if s > 0:
                i = t - begin_of[s]

                @pl.when(both(pcol == s, i >= 0, i < counts[s]))
                def _(s=s, i=i):
                    start_both(s, i)

            j = t - computes[s]

            @pl.when(both(inline(s), j >= 0, j < counts[s]))
            def _(s=s, j=j):
                compute(s, j)

        return carry

    stop = jnp.int32(0)
    for s in range(sections):
        stop = jnp.maximum(stop, jnp.where(inline(s), computes[s] + counts[s], 0))
        for k in range(2):
            stop = jnp.maximum(stop, jnp.where(gets[s][k], lates[s][k] + counts[s], 0))
        if s > 0:
            stop = jnp.maximum(stop, jnp.where(pcol == s, begin_of[s] + counts[s], 0))
    lax.fori_loop(0, stop, turn, 0)
    last = sections - 1

    @pl.when(both(pcol > last, jnp.logical_not(inline(last))))
    def _():
        @pl.when(forwards(last))
        def _():
            pass_row(last)

        take_row(last)

        def body(i, carry):
            at = pl.ds(pl.multiple_of(i * width, width), width)
            out_ref[at, :] = update(last, at)
            return carry

        lax.fori_loop(blocks - live(last), blocks, body, 0)

    save = pltpu.make_async_copy(out_ref, final_ref, local_sem.at[0])
    save.start()
    for s in range(sections):
        for chunk in range(tiles):
            top_flows[s].finish(chunk)

        @pl.when(pcol > s)
        def _(s=s):
            for chunk in range(tiles):
                row_flows[s].finish(chunk)

        owner = s // CORES

        @pl.when(core != s % CORES)
        def _(s=s):
            pick_copy(s, 0, 0, partner).wait_send()

        @pl.when(both(core == s % CORES, x != owner))
        def _(s=s):
            pick_copy(s, 0, 1, partner).wait_send()

        for k in range(2):
            for way in range(4):
                for count in (blocks - 1, blocks):

                    @pl.when(both(sends[s][k][way], live(s) == count))
                    def _(s=s, k=k, way=way, count=count):
                        piece = pl.ds(0, count * width // 2)
                        pltpu.make_async_remote_copy(
                            src_ref=col_panel.at[s, piece],
                            dst_ref=col_panel.at[s, piece],
                            send_sem=col_send.at[s, k, way],
                            recv_sem=col_recv.at[s, k, 0],
                            device_id=ways[way][1],
                            device_id_type=MESH,
                        ).wait_send()

    save.wait()


def on_device(matrix, pivots, lower_inv, upper_inv):
    prow_count = lax.axis_size("prow")
    pcol_count = lax.axis_size("pcol")
    tile = matrix[0, 0]
    rows, width = tile.shape
    sections = pivots.shape[0]
    blocks = rows // width
    assert width == pivots.shape[1] and sections <= prow_count and sections <= pcol_count
    tiles = 3
    relays = blocks * 6
    dma = pltpu.SemaphoreType.DMA
    args = (tile, pivots, lower_inv, upper_inv)
    out = pl.pallas_call(
        functools.partial(factor_kernel, prow_count, pcol_count, sections, width, blocks),
        out_shape=jax.ShapeDtypeStruct(tile.shape, tile.dtype),
        in_specs=[pl.BlockSpec(memory_space=pl.ANY)] * 4,
        out_specs=pl.BlockSpec(memory_space=pl.ANY),
        scratch_shapes=[
            pltpu.VMEM((rows, width), F32),
            pltpu.VMEM((rows, width), F32),
            pltpu.VMEM(pivots.shape, jnp.int32),
            pltpu.VMEM((width, width), F32),
            pltpu.VMEM((width, width), F32),
            pltpu.VMEM((3, rows, width), BF16),
            pltpu.VMEM((sections * width, width), F32),
            pltpu.VMEM((3, sections * width, width), BF16),
            pltpu.VMEM((sections, width, width), F32),
            pltpu.VMEM((sections, 3, width, width), F32),
            pltpu.VMEM((sections, width, width), F32),
            pltpu.VMEM((sections, rows, width), F32),
            pltpu.VMEM((sections, 3 * width, width), BF16),
            pltpu.VMEM((width, 3 * width), BF16),
            pltpu.VMEM((3 * width, width), BF16),
            pltpu.VMEM((3 * width, width), BF16),
            dma((5,)),
            dma((sections, 3, tiles)),
            dma((sections, tiles)),
            dma((sections, 2)),
            dma((sections, 3)),
            dma((sections, 3, tiles)),
            dma((sections, tiles)),
            dma((sections, 2, 4)),
            dma((sections, 2, relays)),
        ],
        compiler_params=pltpu.CompilerParams(
            collective_id=0, has_side_effects=True, vmem_limit_bytes=40 * 1024 * 1024
        ),
    )(*[pltpu.with_memory_space_constraint(v, pltpu.HBM) for v in args])
    return out[None, None]


def solution(mesh):
    return jax.shard_map(
        on_device,
        mesh=mesh,
        in_specs=(P("prow", "pcol", None, None), P(), P(), P()),
        out_specs=P("prow", "pcol", None, None),
        check_vma=False,
    )
```

```python
import functools

import jax
import jax.numpy as jnp
from jax import lax
from jax.experimental import pallas as pl
from jax.experimental.pallas import tpu as pltpu
from jax.sharding import PartitionSpec as P

MESH = pl.DeviceIdType.MESH
CORES = 2
F32 = jnp.float32
BF16 = jnp.bfloat16
HOP = 3
EARLY = (4, 0)
PARTS = 1
PICK = 384
PATIENCE = 4
LAG = 2


def grid_width(count):
    width = 1
    while (2 * width) * (2 * width) <= count:
        width *= 2
    return width if count % width == 0 else 1


def both(*conds):
    out = conds[0]
    for cond in conds[1:]:
        out = jnp.logical_and(out, cond)
    return out


def entry_barrier(neighbours):
    barrier = pltpu.get_barrier_semaphore()
    total = jnp.int32(0)
    for cond, device in neighbours:
        total = total + jnp.where(cond, 1, 0).astype(jnp.int32)

        @pl.when(cond)
        def _(device=device):
            pl.semaphore_signal(barrier, inc=1, device_id=device, device_id_type=MESH)

    pl.semaphore_wait(barrier, total)


def line_ways(prow, prow_count):
    x, core = prow // CORES, prow % CORES
    chips = prow_count // CORES
    return [
        (x + 1 < chips, {"prow": prow + CORES}),
        (x > 0, {"prow": prow - CORES}),
        (prow >= 0, {"prow": x * CORES + (CORES - 1 - core)}),
    ]


def line_sends(prow, prow_count, source):
    x, core = prow // CORES, prow % CORES
    ways = line_ways(prow, prow_count)
    sx, sc = source // CORES, source % CORES
    return [
        (both(ways[0][0], core == sc, x >= sx), ways[0][1]),
        (both(ways[1][0], core == sc, x <= sx), ways[1][1]),
        (core == sc, ways[2][1]),
    ]


def grid_ways(pcol, pcol_count):
    width = grid_width(pcol_count)
    height = pcol_count // width
    z, y = pcol // width, pcol % width
    return [
        (z + 1 < height, {"pcol": pcol + width}),
        (z > 0, {"pcol": pcol - width}),
        (y + 1 < width, {"pcol": pcol + 1}),
        (y > 0, {"pcol": pcol - 1}),
    ]


def tree_plan(pcol_count, source, first_axis):
    width = grid_width(pcol_count)
    extent = (pcol_count // width, width)
    src = (source // width, source % width)
    a, b = first_axis, 1 - first_axis
    near = src[a] + 1 if src[a] + 1 < extent[a] else src[a] - 1

    def toward(at, goal):
        return at + (goal > at) - (goal < at)

    parent = {}
    for node in range(pcol_count):
        pos = [node // width, node % width]
        if node == source:
            continue
        if pos[b] == src[b]:
            pos[a] = toward(pos[a], src[a])
        elif pos[a] != src[a] or extent[a] == 1:
            pos[b] = toward(pos[b], src[b])
        else:
            pos[a] = near
        parent[node] = pos[0] * width + pos[1]
    hops, used = {source: 0}, set()
    for node in range(pcol_count):
        path = [node]
        while path[-1] != source:
            path.append(parent[path[-1]])
        hops[node] = len(path) - 1
        if node > source:
            used.update(path)
    steps = (width, -width, 1, -1)
    senders = [
        [parent[c] for c in used if c != source and c - parent[c] == step]
        if step not in steps[:way] else []
        for way, step in enumerate(steps)
    ]
    return hops, used - {source}, senders


def pick_static(index, table):
    out = jnp.int32(0)
    for key, value in table.items():
        out = jnp.where(index == key, value, out)
    return out


def among(index, members):
    mask = sum(1 << member for member in set(members))
    return (lax.shift_right_logical(jnp.int32(mask), index) & 1) == 1


class Flow:
    def __init__(self, mine, start_ref, land_ref, sends, send_sem, recv_sem, rows):
        self.mine, self.start_ref, self.land_ref = mine, start_ref, land_ref
        self.sends, self.send_sem, self.recv_sem, self.rows = sends, send_sem, recv_sem, rows

    def copy(self, chunk, way, ref):
        piece = pl.ds(chunk * self.rows, self.rows)
        return pltpu.make_async_remote_copy(
            src_ref=ref.at[piece],
            dst_ref=self.land_ref.at[piece],
            send_sem=self.send_sem.at[way, chunk],
            recv_sem=self.recv_sem.at[chunk],
            device_id=self.sends[way][1],
            device_id_type=MESH,
        )

    def send(self, chunk, ref):
        for way, (cond, _device) in enumerate(self.sends):

            @pl.when(cond)
            def _(way=way):
                self.copy(chunk, way, ref).start()

    def pass_on(self, chunk):
        @pl.when(jnp.logical_not(self.mine))
        def _():
            self.copy(chunk, 0, self.land_ref).wait_recv()
            self.send(chunk, self.land_ref)

    def finish(self, chunk):
        for way, (cond, _device) in enumerate(self.sends):

            @pl.when(cond)
            def _(way=way):
                self.copy(chunk, way, self.land_ref).wait_send()


def split2(value):
    high = value.astype(BF16)
    low = (value - high.astype(F32)).astype(BF16)
    return high, low


def split3(value):
    high = value.astype(BF16)
    rest = value - high.astype(F32)
    middle = rest.astype(BF16)
    low = (rest - middle.astype(F32)).astype(BF16)
    return high, middle, low


def wide(value):
    high, low = split2(value)
    return jnp.concatenate([high, high, low], axis=1)


def dot(left, right):
    return jnp.dot(left, right, preferred_element_type=F32)


def factor_kernel(
    prow_count, pcol_count, sections, width, blocks,
    tile_ref, pivots_ref, lower_ref, upper_ref, final_ref,
    out_ref, first, pivot, low_in, up_in, parts, top, top_parts, picked, picked_in,
    row_panel, col_panel, row_stack, low_wide, up_stack, core_stack,
    local_sem, top_send, top_recv, pick_send, pick_recv,
    row_send, row_recv, col_send, col_recv, gate,
):
    prow = lax.axis_index("prow")
    pcol = lax.axis_index("pcol")
    x, core = prow // CORES, prow % CORES
    chips = prow_count // CORES
    step_rows = width // 3
    tiles = width // step_rows
    relay_rows = PARTS * col_panel.shape[1] // (2 * col_recv.shape[2])
    span = 2 * relay_rows
    per_block = width // span

    load_tile = pltpu.make_async_copy(tile_ref, first, local_sem.at[0])
    load_pivots = pltpu.make_async_copy(pivots_ref, pivot, local_sem.at[1])
    load_pivots.start()
    load_tile.start()
    owns_row = prow < sections
    owns_col = pcol < sections

    @pl.when(owns_row)
    def _():
        pltpu.make_async_copy(lower_ref.at[prow], low_in, local_sem.at[2]).start()

    @pl.when(owns_col)
    def _():
        pltpu.make_async_copy(upper_ref.at[pcol], up_in, local_sem.at[3]).start()

    top_flows = [
        Flow(
            prow == s, tile_ref, top.at[pl.ds(s * width, width)],
            line_sends(prow, prow_count, s), top_send.at[s], top_recv.at[s], step_rows,
        )
        for s in range(sections)
    ]
    row_flows = [
        Flow(
            prow == s, row_panel.at[s], row_panel.at[s],
            line_sends(prow, prow_count, s), row_send.at[s], row_recv.at[s], step_rows,
        )
        for s in range(sections)
    ]

    entry_barrier(line_ways(prow, prow_count) + grid_ways(pcol, pcol_count))

    def waits_for_picks(s):
        return prow >= 0 if s >= CORES else prow < 0

    for s in range(sections):

        @pl.when(prow == s)
        def _(s=s):
            for chunk in range(tiles - 1):
                top_flows[s].send(chunk, tile_ref)

            @pl.when(jnp.logical_not(waits_for_picks(s)))
            def _():
                top_flows[s].send(tiles - 1, tile_ref)

            pltpu.make_async_copy(
                tile_ref.at[pl.ds(0, width)], top.at[pl.ds(s * width, width)], local_sem.at[4]
            ).start()

    def lanes(count):
        return lax.broadcasted_iota(jnp.int32, (1, count), 1).astype(F32)

    def column(start, rows=step_rows):
        ids = lax.broadcasted_iota(jnp.int32, (rows, 1), 0)
        return (ids + start).astype(F32)

    def pivot_row(s):
        return pivot[pl.ds(s, 1), :].astype(F32)

    def undo(rows, upto):
        for s in reversed(range(upto)):
            listed = pivot_row(s)
            shift = lanes(width) + F32(s * width) - listed
            moved = jnp.where(rows == listed, shift, F32(0))
            rows = rows + jnp.sum(moved, axis=1, keepdims=True)
        return rows

    def one_hot(rows, ids):
        return jnp.where(rows == ids, F32(1), F32(0)).astype(BF16)

    load_pivots.wait()
    load_tile.wait()

    def cut_tile(i, carry):
        at = pl.ds(pl.multiple_of(i * step_rows, step_rows), step_rows)
        for k, part in enumerate(split3(first[at, :])):
            parts[k, at, :] = part
        return carry

    lax.fori_loop(0, tiles * blocks, cut_tile, 0)

    def pick_copy(s, slot, where, device):
        return pltpu.make_async_remote_copy(
            src_ref=picked.at[s],
            dst_ref=picked_in.at[s, slot],
            send_sem=pick_send.at[s, where],
            recv_sem=pick_recv.at[s, slot],
            device_id=device,
            device_id_type=MESH,
        )

    partner = {"prow": x * CORES + (CORES - 1 - core)}
    held_ids = jnp.concatenate(
        [
            lanes(width) + ((block * prow_count + prow) * width).astype(F32)
            for block in range(blocks)
        ],
        axis=1,
    )
    def pick_rows(s):
        def pick(i, carry):
            start = i * PICK
            at = pl.ds(pl.multiple_of(start, PICK), PICK)
            rows = jnp.sum(
                jnp.where(column(start, PICK) == lanes(width), pivot_row(s), F32(0)),
                axis=1, keepdims=True,
            )
            chosen = one_hot(undo(rows, s), held_ids)
            picked[s, at, :] = (
                dot(chosen, parts[2]) + dot(chosen, parts[1]) + dot(chosen, parts[0])
            )
            return carry

        lax.fori_loop(0, width // PICK, pick, 0)

        @pl.when(core != s % CORES)
        def _():
            pick_copy(s, 0, 0, partner).start()

    def add_in(s, slot):
        pick_copy(s, slot, 1, partner).wait_recv()

        def add(i, carry):
            at = pl.ds(pl.multiple_of(i * step_rows, step_rows), step_rows)
            picked[s, at, :] += picked_in[s, slot, at, :]
            return carry

        lax.fori_loop(0, tiles, add, 0)

    def pass_picked(s, when):
        owner = s // CORES

        @pl.when(both(core == s % CORES, x != owner, when))
        def _():
            add_in(s, 0)

            @pl.when(both(x < owner, x > 0))
            def _():
                add_in(s, 1)

            @pl.when(both(x > owner, x < chips - 1))
            def _():
                add_in(s, 2)

            @pl.when(x < owner)
            def _():
                pick_copy(s, 1, 1, {"prow": prow + CORES}).start()

            @pl.when(x > owner)
            def _():
                pick_copy(s, 2, 1, {"prow": prow - CORES}).start()

    def urgent(s):
        return pcol > 0 if s == 0 else pcol == 0

    def pick_all(order):
        for s in order:
            pick_rows(s)
            pass_picked(s, urgent(s))

    @pl.when(pcol == 0)
    def _():
        pick_all([*range(1, sections), 0])

    @pl.when(pcol > 0)
    def _():
        pick_all([*range(sections)])

    for s in range(sections):

        @pl.when(both(prow == s, waits_for_picks(s)))
        def _(s=s):
            top_flows[s].send(tiles - 1, tile_ref)


    @pl.when(owns_row)
    def _():
        pltpu.make_async_copy(lower_ref.at[prow], low_in, local_sem.at[2]).wait()

        def prepare(i, carry):
            start = i * step_rows
            at = pl.ds(pl.multiple_of(start, step_rows), step_rows)
            below = column(start) > lanes(width)
            same = column(start) == lanes(width)
            unit = jnp.where(below, low_in[at, :], jnp.where(same, F32(1), F32(0)))
            low_wide[at, :] = wide(unit)
            return carry

        lax.fori_loop(0, tiles, prepare, 0)

    def stack(ref, i, value):
        high, low = split2(value)
        start = i * step_rows
        for k, part in enumerate((high, low, high)):
            at = pl.ds(pl.multiple_of(k * width + start, step_rows), step_rows)
            ref[at, :] = part

    @pl.when(owns_col)
    def _():
        pltpu.make_async_copy(upper_ref.at[pcol], up_in, local_sem.at[3]).wait()

        def prepare(i, carry):
            start = i * step_rows
            at = pl.ds(pl.multiple_of(start, step_rows), step_rows)
            kept = jnp.where(column(start) <= lanes(width), up_in[at, :], F32(0))
            stack(up_stack, i, kept)
            return carry

        lax.fori_loop(0, tiles, prepare, 0)

    def take_picked(s):
        owner = s // CORES
        add_in(s, 0)
        if owner > 0:
            add_in(s, 1)
        if owner < chips - 1:
            add_in(s, 2)
        out_ref[pl.ds(0, width), :] = picked[s]

    ways = grid_ways(pcol, pcol_count)
    plans = [[tree_plan(pcol_count, s, k) for k in range(2)] for s in range(sections)]
    sends = [[[among(pcol, who) for who in plan[2]] for plan in pair] for pair in plans]
    gets = [[among(pcol, plan[1]) for plan in pair] for pair in plans]

    def farthest(s, node):
        return max(plan[0][node] for plan in plans[s])

    def live(s):
        return jnp.where(prow > s, blocks, blocks - 1)

    def place_of(s, i):
        turn = lax.div(i, per_block)
        block = blocks - live(s) + turn
        return block * width + (i - turn * per_block) * span

    part_rows = relay_rows // PARTS

    def col_copy(s, k, i, h, way):
        start = place_of(s, i) + k * relay_rows + h * part_rows
        piece = pl.ds(pl.multiple_of(start, part_rows), part_rows)
        return pltpu.make_async_remote_copy(
            src_ref=col_panel.at[s, piece],
            dst_ref=col_panel.at[s, piece],
            send_sem=col_send.at[s, k, way],
            recv_sem=col_recv.at[s, k, i * PARTS + h],
            device_id=ways[way][1],
            device_id_type=MESH,
        )

    def col_start(s, k, i, h):
        for way in range(4):

            @pl.when(sends[s][k][way])
            def _(way=way):
                col_copy(s, k, i, h, way).start()

    def update(s, at):
        return out_ref[at, :] - dot(wide(col_panel[s, at, :]), row_stack[s])

    def rows_of(s, i):
        return pl.ds(pl.multiple_of(place_of(s, i), span), span)

    def produce(s, i, value):
        at = rows_of(s, i)
        value = dot(wide(value), up_stack[...])
        col_panel[s, at, :] = value
        out_ref[at, :] = value

    def start_both(s, i):
        for h in range(PARTS):
            for k in range(2):
                col_start(s, k, i, h)

    def produce_first(start, stop):
        def body(i, carry):
            produce(0, i, out_ref[rows_of(0, i), :])

            @pl.when(i > start)
            def _():
                start_both(0, i - 1)

            return carry

        lax.fori_loop(start, stop, body, 0)
        start_both(0, stop - 1)

    for s in range(1, min(CORES, sections)):

        @pl.when(both(pcol == 0, prow == s))
        def _(s=s):
            take_picked(s)
            produce_first(0, per_block)
            pl.semaphore_signal(gate, inc=1, device_id=partner, device_id_type=MESH)

    def row_product(s, chunk):
        at = pl.ds(chunk * step_rows, step_rows)
        stack(core_stack, chunk, out_ref[at, :])
        upto = (chunk + 1) * step_rows
        value = F32(0)
        for k in range(3):
            upper = pl.ds(k * width, upto)
            value = value + dot(low_wide[at, k * width : k * width + upto], core_stack[upper, :])
        row_panel[s, at, :] = value
        out_ref[at, :] = value

    @pl.when(both(prow == 0, pcol > 0))
    def _():
        take_picked(0)
        for chunk in range(tiles):
            row_product(0, chunk)
            if chunk > 0:
                row_flows[0].send(chunk - 1, row_panel.at[0])
        row_flows[0].send(tiles - 1, row_panel.at[0])

    later = both(prow > 0, prow < min(CORES, sections), pcol > 0)

    def land_tops():
        for chunk in range(tiles):
            for flow in top_flows:
                flow.pass_on(chunk)
            if chunk == tiles - 2:
                for s in range(sections):
                    pass_picked(s, jnp.logical_not(urgent(s)))
        for s in range(sections):

            @pl.when(prow == s)
            def _(s=s):
                pltpu.make_async_copy(
                    tile_ref.at[pl.ds(0, width)], top.at[pl.ds(s * width, width)], local_sem.at[4]
                ).wait()

        def cut_top(i, carry):
            at = pl.ds(pl.multiple_of(i * step_rows, step_rows), step_rows)
            for k, part in enumerate(split3(top[at, :])):
                top_parts[k, at, :] = part
            return carry

        lax.fori_loop(0, tiles * sections, cut_top, 0)

    pl.when(jnp.logical_not(later))(land_tops)

    def settle(block):
        def place(i, carry):
            start = i * PICK
            at = pl.ds(pl.multiple_of(block * width + start, PICK), PICK)
            rows = column(start + (block * prow_count + prow) * width, PICK)
            rows = undo(rows, sections)
            chosen = one_hot(rows, lanes(sections * width))
            value = (
                dot(chosen, top_parts[2]) + dot(chosen, top_parts[1]) + dot(chosen, top_parts[0])
            )
            out_ref[at, :] = jnp.where(rows < F32(sections * width), value, first[at, :])
            return carry

        lax.fori_loop(0, width // PICK, place, 0)

    def forwards(s):
        return both(core == s % CORES, prow != s)

    def pass_row(s):
        for chunk in range(tiles):
            row_flows[s].pass_on(chunk)

    def take_row(s):
        @pl.when(jnp.logical_not(forwards(s)))
        def _():
            pass_row(s)

        def cut(i, carry):
            at = pl.ds(pl.multiple_of(i * step_rows, step_rows), step_rows)
            stack(row_stack.at[s], i, row_panel[s, at, :])
            return carry

        lax.fori_loop(0, tiles, cut, 0)

    @pl.when(pcol == 0)
    def _():
        @pl.when(jnp.logical_not(owns_row))
        def _():
            settle(0)
            produce_first(0, per_block)

        for block in range(1, blocks):
            settle(block)
        for s in range(CORES, sections):

            @pl.when(prow == s)
            def _(s=s):
                take_picked(s)

        if sections > 1:

            @pl.when(prow == 0)
            def _():
                pl.semaphore_wait(gate, 1)

        paired = [s for s in range(CORES, sections) if s ^ 1 >= sections]
        for s in paired:

            @pl.when(prow == s ^ 1)
            def _():
                pl.semaphore_wait(gate, 1)

        done = jnp.logical_or(both(prow > 0, prow < CORES), jnp.logical_not(owns_row))
        produce_first(jnp.where(done, per_block, 0), live(0) * per_block)
        for s in paired:

            @pl.when(prow == s)
            def _():
                pl.semaphore_signal(gate, inc=1, device_id=partner, device_id_type=MESH)

    @pl.when(both(pcol > 0, jnp.logical_not(later)))
    def _():
        for block in range(1, blocks):
            settle(block)

        @pl.when(jnp.logical_not(owns_row))
        def _():
            settle(0)

    begin, begin_of, lates, computes, counts = jnp.int32(0), [], [], [], []
    forward_at = []
    for s in range(sections):
        counts.append(live(s) * per_block)
        begin_of.append(begin)
        lates.append(
            [begin + pick_static(pcol, {n: HOP * h for n, h in plan[0].items()}) for plan in plans[s]]
        )
        lag = {n: HOP * farthest(s, n) + (LAG if n != s + 1 else 0) for n in range(pcol_count)}
        slack = jnp.where(x == 0, per_block, 0) if s == 0 else 0
        rest = PATIENCE if s == 0 else 0
        wait = jnp.where(both(prow >= CORES, prow < sections, pcol != 1), rest, 0)
        early = {n: HOP * farthest(s, n) - EARLY[min(s, 1)] for n in range(pcol_count)}
        forward_at.append(begin + pick_static(pcol, early))
        computes.append(begin + pick_static(pcol, lag) + jnp.where(pcol == s + 1, slack, wait))
        if s + 1 < sections:
            begin = begin + HOP * farthest(s, s + 1) + 1 + slack
            begin = begin + jnp.where(prow == s + 1, per_block, 0)
            for n in range(s + 2, pcol_count):
                ahead = HOP * (farthest(s, s + 1) + farthest(s + 1, n) - farthest(s, n))
                assert ahead + 1 >= (LAG if n == s + 2 else 0) + rest

    def inline(s):
        return pcol < 0 if s + 1 == sections else pcol > s

    def compute(s, j):
        last = s + 1 == sections
        skip = 0 if last else counts[s] - counts[s + 1]

        @pl.when(j == 0)
        def _():
            if s == 0:
                for other in range(1, sections):

                    @pl.when(prow == other)
                    def _(other=other):
                        take_picked(other)

            take_row(s)

        if s == 0:

            @pl.when(both(later, j == per_block))
            def _():
                land_tops()
                for block in range(1, blocks):
                    settle(block)

        at = rows_of(s, j)
        value = update(s, at)
        if last:
            out_ref[at, :] = value
            return
        makes = both(pcol == s + 1, j >= skip)

        @pl.when(jnp.logical_not(makes))
        def _():
            out_ref[at, :] = value

        @pl.when(makes)
        def _():
            produce(s + 1, j - skip, value)

        per_tile = per_block // tiles
        for chunk in range(tiles):
            ready = (chunk + 1) * per_tile - 1

            @pl.when(both(prow == s + 1, pcol > s + 1, j == ready))
            def _(chunk=chunk):
                row_product(s + 1, chunk)
                if chunk == tiles - 1:
                    row_flows[s + 1].send(chunk, row_panel.at[s + 1])

            if chunk < tiles - 1:

                @pl.when(both(prow == s + 1, pcol > s + 1, j == ready + 1))
                def _(chunk=chunk):
                    row_flows[s + 1].send(chunk, row_panel.at[s + 1])

    def turn(t, carry):
        for s in range(sections):
            for k in range(2):
                i = t - lates[s][k]

                @pl.when(both(gets[s][k], i >= 0, i < counts[s]))
                def _(s=s, k=k, i=i):
                    for h in range(PARTS):
                        col_copy(s, k, i, h, 0).wait_recv()
                        col_start(s, k, i, h)

            @pl.when(both(inline(s), forwards(s), t == jnp.maximum(forward_at[s], 0)))
            def _(s=s):
                pass_row(s)

            if s > 0:
                i = t - begin_of[s]

                @pl.when(both(pcol == s, i >= 0, i < counts[s]))
                def _(s=s, i=i):
                    start_both(s, i)

            j = t - computes[s]

            @pl.when(both(inline(s), j >= 0, j < counts[s]))
            def _(s=s, j=j):
                compute(s, j)

        return carry

    stop = jnp.int32(0)
    for s in range(sections):
        stop = jnp.maximum(stop, jnp.where(inline(s), computes[s] + counts[s], 0))
        for k in range(2):
            stop = jnp.maximum(stop, jnp.where(gets[s][k], lates[s][k] + counts[s], 0))
        if s > 0:
            stop = jnp.maximum(stop, jnp.where(pcol == s, begin_of[s] + counts[s], 0))
    lax.fori_loop(0, stop, turn, 0)
    last = sections - 1

    @pl.when(both(prow == 0, pcol == 0))
    def _():
        take_picked(0)

    @pl.when(both(pcol > last, jnp.logical_not(inline(last))))
    def _():
        @pl.when(forwards(last))
        def _():
            pass_row(last)

        take_row(last)

        def body(i, carry):
            at = pl.ds(pl.multiple_of(i * width, width), width)
            out_ref[at, :] = update(last, at)
            return carry

        lax.fori_loop(blocks - live(last), blocks, body, 0)

    save = pltpu.make_async_copy(out_ref, final_ref, local_sem.at[0])
    save.start()
    for s in range(sections):
        for chunk in range(tiles):
            top_flows[s].finish(chunk)

        @pl.when(pcol > s)
        def _(s=s):
            for chunk in range(tiles):
                row_flows[s].finish(chunk)

        owner = s // CORES

        @pl.when(core != s % CORES)
        def _(s=s):
            pick_copy(s, 0, 0, partner).wait_send()

        @pl.when(both(core == s % CORES, x != owner))
        def _(s=s):
            pick_copy(s, 0, 1, partner).wait_send()

        for k in range(2):
            for way in range(4):
                for count in (blocks - 1, blocks):

                    @pl.when(both(sends[s][k][way], live(s) == count))
                    def _(s=s, k=k, way=way, count=count):
                        piece = pl.ds(0, count * width // 2)
                        pltpu.make_async_remote_copy(
                            src_ref=col_panel.at[s, piece],
                            dst_ref=col_panel.at[s, piece],
                            send_sem=col_send.at[s, k, way],
                            recv_sem=col_recv.at[s, k, 0],
                            device_id=ways[way][1],
                            device_id_type=MESH,
                        ).wait_send()

    save.wait()


def on_device(matrix, pivots, lower_inv, upper_inv):
    prow_count = lax.axis_size("prow")
    pcol_count = lax.axis_size("pcol")
    tile = matrix[0, 0]
    rows, width = tile.shape
    sections = pivots.shape[0]
    blocks = rows // width
    assert width == pivots.shape[1] and sections <= prow_count and sections <= pcol_count
    tiles = 3
    relays = blocks * 6
    dma = pltpu.SemaphoreType.DMA
    args = (tile, pivots, lower_inv, upper_inv)
    out = pl.pallas_call(
        functools.partial(factor_kernel, prow_count, pcol_count, sections, width, blocks),
        out_shape=jax.ShapeDtypeStruct(tile.shape, tile.dtype),
        in_specs=[pl.BlockSpec(memory_space=pl.ANY)] * 4,
        out_specs=pl.BlockSpec(memory_space=pl.ANY),
        scratch_shapes=[
            pltpu.VMEM((rows, width), F32),
            pltpu.VMEM((rows, width), F32),
            pltpu.VMEM(pivots.shape, jnp.int32),
            pltpu.VMEM((width, width), F32),
            pltpu.VMEM((width, width), F32),
            pltpu.VMEM((3, rows, width), BF16),
            pltpu.VMEM((sections * width, width), F32),
            pltpu.VMEM((3, sections * width, width), BF16),
            pltpu.VMEM((sections, width, width), F32),
            pltpu.VMEM((sections, 3, width, width), F32),
            pltpu.VMEM((sections, width, width), F32),
            pltpu.VMEM((sections, rows, width), F32),
            pltpu.VMEM((sections, 3 * width, width), BF16),
            pltpu.VMEM((width, 3 * width), BF16),
            pltpu.VMEM((3 * width, width), BF16),
            pltpu.VMEM((3 * width, width), BF16),
            dma((5,)),
            dma((sections, 3, tiles)),
            dma((sections, tiles)),
            dma((sections, 2)),
            dma((sections, 3)),
            dma((sections, 3, tiles)),
            dma((sections, tiles)),
            dma((sections, 2, 4)),
            dma((sections, 2, relays * PARTS)),
            pltpu.SemaphoreType.REGULAR,
        ],
        compiler_params=pltpu.CompilerParams(
            collective_id=0, has_side_effects=True, vmem_limit_bytes=40 * 1024 * 1024
        ),
    )(*[pltpu.with_memory_space_constraint(v, pltpu.HBM) for v in args])
    return out[None, None]


def solution(mesh):
    return jax.shard_map(
        on_device,
        mesh=mesh,
        in_specs=(P("prow", "pcol", None, None), P(), P(), P()),
        out_specs=P("prow", "pcol", None, None),
        check_vma=False,
    )
```

```python
import functools

import jax
import jax.numpy as jnp
from jax import lax
from jax.experimental import pallas as pl
from jax.experimental.pallas import tpu as pltpu
from jax.sharding import PartitionSpec as P

MESH = pl.DeviceIdType.MESH
CORES = 2
F32 = jnp.float32
BF16 = jnp.bfloat16
HOP = 3
EARLY = (4, 0)
PARTS = 1
PATIENCE = 4
LAG = 2


def grid_width(count):
    width = 1
    while (2 * width) * (2 * width) <= count:
        width *= 2
    return width if count % width == 0 else 1


def both(*conds):
    out = conds[0]
    for cond in conds[1:]:
        out = jnp.logical_and(out, cond)
    return out


def entry_barrier(neighbours):
    barrier = pltpu.get_barrier_semaphore()
    total = jnp.int32(0)
    for cond, device in neighbours:
        total = total + jnp.where(cond, 1, 0).astype(jnp.int32)

        @pl.when(cond)
        def _(device=device):
            pl.semaphore_signal(barrier, inc=1, device_id=device, device_id_type=MESH)

    pl.semaphore_wait(barrier, total)


def line_ways(prow, prow_count):
    x, core = prow // CORES, prow % CORES
    chips = prow_count // CORES
    return [
        (x + 1 < chips, {"prow": prow + CORES}),
        (x > 0, {"prow": prow - CORES}),
        (prow >= 0, {"prow": x * CORES + (CORES - 1 - core)}),
    ]


def line_sends(prow, prow_count, source):
    x, core = prow // CORES, prow % CORES
    ways = line_ways(prow, prow_count)
    sx, sc = source // CORES, source % CORES
    return [
        (both(ways[0][0], core == sc, x >= sx), ways[0][1]),
        (both(ways[1][0], core == sc, x <= sx), ways[1][1]),
        (core == sc, ways[2][1]),
    ]


def grid_ways(pcol, pcol_count):
    width = grid_width(pcol_count)
    height = pcol_count // width
    z, y = pcol // width, pcol % width
    return [
        (z + 1 < height, {"pcol": pcol + width}),
        (z > 0, {"pcol": pcol - width}),
        (y + 1 < width, {"pcol": pcol + 1}),
        (y > 0, {"pcol": pcol - 1}),
    ]


def tree_plan(pcol_count, source, first_axis):
    width = grid_width(pcol_count)
    extent = (pcol_count // width, width)
    src = (source // width, source % width)
    a, b = first_axis, 1 - first_axis
    near = src[a] + 1 if src[a] + 1 < extent[a] else src[a] - 1

    def toward(at, goal):
        return at + (goal > at) - (goal < at)

    parent = {}
    for node in range(pcol_count):
        pos = [node // width, node % width]
        if node == source:
            continue
        if pos[b] == src[b]:
            pos[a] = toward(pos[a], src[a])
        elif pos[a] != src[a] or extent[a] == 1:
            pos[b] = toward(pos[b], src[b])
        else:
            pos[a] = near
        parent[node] = pos[0] * width + pos[1]
    hops, used = {source: 0}, set()
    for node in range(pcol_count):
        path = [node]
        while path[-1] != source:
            path.append(parent[path[-1]])
        hops[node] = len(path) - 1
        if node > source:
            used.update(path)
    steps = (width, -width, 1, -1)
    senders = [
        [parent[c] for c in used if c != source and c - parent[c] == step]
        if step not in steps[:way] else []
        for way, step in enumerate(steps)
    ]
    return hops, used - {source}, senders


def pick_static(index, table):
    out = jnp.int32(0)
    for key, value in table.items():
        out = jnp.where(index == key, value, out)
    return out


def among(index, members):
    mask = sum(1 << member for member in set(members))
    return (lax.shift_right_logical(jnp.int32(mask), index) & 1) == 1


class Flow:
    def __init__(self, mine, start_ref, land_ref, sends, send_sem, recv_sem, rows):
        self.mine, self.start_ref, self.land_ref = mine, start_ref, land_ref
        self.sends, self.send_sem, self.recv_sem, self.rows = sends, send_sem, recv_sem, rows

    def copy(self, chunk, way, ref):
        piece = pl.ds(chunk * self.rows, self.rows)
        return pltpu.make_async_remote_copy(
            src_ref=ref.at[piece],
            dst_ref=self.land_ref.at[piece],
            send_sem=self.send_sem.at[way],
            recv_sem=self.recv_sem.at[chunk],
            device_id=self.sends[way][1],
            device_id_type=MESH,
        )

    def send(self, chunk, ref):
        for way, (cond, _device) in enumerate(self.sends):

            @pl.when(cond)
            def _(way=way):
                self.copy(chunk, way, ref).start()

    def pass_on(self, chunk):
        @pl.when(jnp.logical_not(self.mine))
        def _():
            self.copy(chunk, 0, self.land_ref).wait_recv()
            self.send(chunk, self.land_ref)

    def finish(self, count):
        piece = pl.ds(0, count * self.rows)
        for way, (cond, device) in enumerate(self.sends):

            @pl.when(cond)
            def _(way=way, device=device):
                pltpu.make_async_remote_copy(
                    src_ref=self.land_ref.at[piece],
                    dst_ref=self.land_ref.at[piece],
                    send_sem=self.send_sem.at[way],
                    recv_sem=self.recv_sem.at[0],
                    device_id=device,
                    device_id_type=MESH,
                ).wait_send()


def split2(value):
    high = value.astype(BF16)
    low = (value - high.astype(F32)).astype(BF16)
    return high, low


def split3(value):
    high = value.astype(BF16)
    rest = value - high.astype(F32)
    middle = rest.astype(BF16)
    low = (rest - middle.astype(F32)).astype(BF16)
    return high, middle, low


def wide(value):
    high, low = split2(value)
    return jnp.concatenate([high, high, low], axis=1)


def dot(left, right):
    return jnp.dot(left, right, preferred_element_type=F32)


def factor_kernel(
    prow_count, pcol_count, sections, width, blocks,
    tile_ref, pivots_ref, lower_ref, upper_ref, final_ref,
    out_ref, first, pivot, low_in, up_in, parts, top, top_parts, picked, picked_in,
    row_panel, col_panel, row_stack, low_wide, up_stack, core_stack,
    local_sem, top_send, top_recv, pick_send, pick_recv,
    row_send, row_recv, col_send, col_recv, gate,
):
    prow = lax.axis_index("prow")
    pcol = lax.axis_index("pcol")
    x, core = prow // CORES, prow % CORES
    chips = prow_count // CORES
    step_rows = width // 3
    tiles = width // step_rows
    relay_rows = PARTS * col_panel.shape[1] // (2 * col_recv.shape[2])
    span = 2 * relay_rows
    per_block = width // span

    load_tile = pltpu.make_async_copy(tile_ref, first, local_sem.at[0])
    load_pivots = pltpu.make_async_copy(pivots_ref, pivot, local_sem.at[1])
    load_pivots.start()
    load_tile.start()
    owns_row = prow < sections
    owns_col = pcol < sections

    @pl.when(owns_row)
    def _():
        pltpu.make_async_copy(lower_ref.at[prow], low_in, local_sem.at[2]).start()

    @pl.when(owns_col)
    def _():
        pltpu.make_async_copy(upper_ref.at[pcol], up_in, local_sem.at[3]).start()

    top_flows = [
        Flow(
            prow == s, tile_ref, top.at[pl.ds(s * width, width)],
            line_sends(prow, prow_count, s), top_send.at[s], top_recv.at[s], step_rows,
        )
        for s in range(sections)
    ]
    row_flows = [
        Flow(
            prow == s, row_panel.at[s], row_panel.at[s],
            line_sends(prow, prow_count, s), row_send.at[s], row_recv.at[s], step_rows,
        )
        for s in range(sections)
    ]

    entry_barrier(line_ways(prow, prow_count) + grid_ways(pcol, pcol_count))

    def waits_for_picks(s):
        return prow >= 0 if s >= CORES else prow < 0

    for s in range(sections):

        @pl.when(prow == s)
        def _(s=s):
            for chunk in range(tiles - 1):
                top_flows[s].send(chunk, tile_ref)

            @pl.when(jnp.logical_not(waits_for_picks(s)))
            def _():
                top_flows[s].send(tiles - 1, tile_ref)

            pltpu.make_async_copy(
                tile_ref.at[pl.ds(0, width)], top.at[pl.ds(s * width, width)], local_sem.at[4]
            ).start()

    def lanes(count):
        return lax.broadcasted_iota(jnp.int32, (1, count), 1).astype(F32)

    def column(start, rows=step_rows):
        ids = lax.broadcasted_iota(jnp.int32, (rows, 1), 0)
        return (ids + start).astype(F32)

    def pivot_row(s):
        return pivot[pl.ds(s, 1), :].astype(F32)

    def undo(rows, upto):
        for s in reversed(range(upto)):
            listed = pivot_row(s)
            shift = lanes(width) + F32(s * width) - listed
            moved = jnp.where(rows == listed, shift, F32(0))
            rows = rows + jnp.sum(moved, axis=1, keepdims=True)
        return rows

    def one_hot(rows, ids):
        return jnp.where(rows == ids, F32(1), F32(0)).astype(BF16)

    load_pivots.wait()
    load_tile.wait()

    def cut_tile(i, carry):
        at = pl.ds(pl.multiple_of(i * step_rows, step_rows), step_rows)
        for k, part in enumerate(split3(first[at, :])):
            parts[k, at, :] = part
        return carry

    lax.fori_loop(0, tiles * blocks, cut_tile, 0)

    def pick_copy(s, slot, where, device):
        return pltpu.make_async_remote_copy(
            src_ref=picked.at[s],
            dst_ref=picked_in.at[s, slot],
            send_sem=pick_send.at[s, where],
            recv_sem=pick_recv.at[s, slot],
            device_id=device,
            device_id_type=MESH,
        )

    partner = {"prow": x * CORES + (CORES - 1 - core)}
    held_ids = jnp.concatenate(
        [
            lanes(width) + ((block * prow_count + prow) * width).astype(F32)
            for block in range(blocks)
        ],
        axis=1,
    )
    def pick_rows(s):
        def pick(i, carry):
            start = i * width
            at = pl.ds(pl.multiple_of(start, width), width)
            rows = jnp.sum(
                jnp.where(column(start, width) == lanes(width), pivot_row(s), F32(0)),
                axis=1, keepdims=True,
            )
            chosen = one_hot(undo(rows, s), held_ids)
            picked[s, at, :] = (
                dot(chosen, parts[2]) + dot(chosen, parts[1]) + dot(chosen, parts[0])
            )
            return carry

        lax.fori_loop(0, width // width, pick, 0)

        @pl.when(core != s % CORES)
        def _():
            pick_copy(s, 0, 0, partner).start()

    def add_in(s, slot):
        pick_copy(s, slot, 1, partner).wait_recv()

        def add(i, carry):
            at = pl.ds(pl.multiple_of(i * step_rows, step_rows), step_rows)
            picked[s, at, :] += picked_in[s, slot, at, :]
            return carry

        lax.fori_loop(0, tiles, add, 0)

    def pass_picked(s, when):
        owner = s // CORES

        @pl.when(both(core == s % CORES, x != owner, when))
        def _():
            add_in(s, 0)

            @pl.when(both(x < owner, x > 0))
            def _():
                add_in(s, 1)

            @pl.when(both(x > owner, x < chips - 1))
            def _():
                add_in(s, 2)

            @pl.when(x < owner)
            def _():
                pick_copy(s, 1, 1, {"prow": prow + CORES}).start()

            @pl.when(x > owner)
            def _():
                pick_copy(s, 2, 1, {"prow": prow - CORES}).start()

    def urgent(s):
        return pcol > 0 if s == 0 else pcol == 0

    def pick_all(order):
        for s in order:
            pick_rows(s)
            pass_picked(s, urgent(s))

    @pl.when(pcol == 0)
    def _():
        pick_all([*range(1, sections), 0])

    @pl.when(pcol > 0)
    def _():
        pick_all([*range(sections)])

    for s in range(sections):

        @pl.when(both(prow == s, waits_for_picks(s)))
        def _(s=s):
            top_flows[s].send(tiles - 1, tile_ref)


    @pl.when(owns_row)
    def _():
        pltpu.make_async_copy(lower_ref.at[prow], low_in, local_sem.at[2]).wait()

        def prepare(i, carry):
            start = i * step_rows
            at = pl.ds(pl.multiple_of(start, step_rows), step_rows)
            below = column(start) > lanes(width)
            same = column(start) == lanes(width)
            unit = jnp.where(below, low_in[at, :], jnp.where(same, F32(1), F32(0)))
            low_wide[at, :] = wide(unit)
            return carry

        lax.fori_loop(0, tiles, prepare, 0)

    def stack(ref, i, value):
        high, low = split2(value)
        start = i * step_rows
        for k, part in enumerate((high, low, high)):
            at = pl.ds(pl.multiple_of(k * width + start, step_rows), step_rows)
            ref[at, :] = part

    @pl.when(owns_col)
    def _():
        pltpu.make_async_copy(upper_ref.at[pcol], up_in, local_sem.at[3]).wait()

        def prepare(i, carry):
            start = i * step_rows
            at = pl.ds(pl.multiple_of(start, step_rows), step_rows)
            kept = jnp.where(column(start) <= lanes(width), up_in[at, :], F32(0))
            stack(up_stack, i, kept)
            return carry

        lax.fori_loop(0, tiles, prepare, 0)

    def take_picked(s):
        owner = s // CORES
        add_in(s, 0)
        slots = [1] * (owner > 0) + [2] * (owner < chips - 1)
        for slot in slots[:-1]:
            add_in(s, slot)
        for slot in slots[-1:]:
            pick_copy(s, slot, 1, partner).wait_recv()

        def put(i, carry):
            at = pl.ds(pl.multiple_of(i * step_rows, step_rows), step_rows)
            value = picked[s, at, :]
            for slot in slots[-1:]:
                value = value + picked_in[s, slot, at, :]
            out_ref[at, :] = value
            return carry

        lax.fori_loop(0, tiles, put, 0)

    ways = grid_ways(pcol, pcol_count)
    plans = [[tree_plan(pcol_count, s, k) for k in range(2)] for s in range(sections)]
    sends = [[[among(pcol, who) for who in plan[2]] for plan in pair] for pair in plans]
    gets = [[among(pcol, plan[1]) for plan in pair] for pair in plans]

    def farthest(s, node):
        return max(plan[0][node] for plan in plans[s])

    def live(s):
        return jnp.where(prow > s, blocks, blocks - 1)

    def place_of(s, i):
        turn = lax.div(i, per_block)
        block = blocks - live(s) + turn
        return block * width + (i - turn * per_block) * span

    part_rows = relay_rows // PARTS

    def col_copy(s, k, i, h, way):
        start = place_of(s, i) + k * relay_rows + h * part_rows
        piece = pl.ds(pl.multiple_of(start, part_rows), part_rows)
        return pltpu.make_async_remote_copy(
            src_ref=col_panel.at[s, piece],
            dst_ref=col_panel.at[s, piece],
            send_sem=col_send.at[s, k, way],
            recv_sem=col_recv.at[s, k, i * PARTS + h],
            device_id=ways[way][1],
            device_id_type=MESH,
        )

    def col_start(s, k, i, h):
        for way in range(4):

            @pl.when(sends[s][k][way])
            def _(way=way):
                col_copy(s, k, i, h, way).start()

    def update(s, at):
        return out_ref[at, :] - dot(wide(col_panel[s, at, :]), row_stack[s])

    def rows_of(s, i):
        return pl.ds(pl.multiple_of(place_of(s, i), span), span)

    def produce(s, i, value):
        at = rows_of(s, i)
        value = dot(wide(value), up_stack[...])
        col_panel[s, at, :] = value
        out_ref[at, :] = value

    def start_both(s, i):
        for h in range(PARTS):
            for k in range(2):
                col_start(s, k, i, h)

    def produce_first(start, stop):
        def body(i, carry):
            produce(0, i, out_ref[rows_of(0, i), :])

            @pl.when(i > start)
            def _():
                start_both(0, i - 1)

            return carry

        lax.fori_loop(start, stop, body, 0)
        start_both(0, stop - 1)

    for s in range(1, min(CORES, sections)):

        @pl.when(both(pcol == 0, prow == s))
        def _(s=s):
            take_picked(s)
            produce_first(0, per_block)
            pl.semaphore_signal(gate, inc=1, device_id=partner, device_id_type=MESH)

    def row_product(s, chunk):
        at = pl.ds(chunk * step_rows, step_rows)
        stack(core_stack, chunk, out_ref[at, :])
        upto = (chunk + 1) * step_rows
        value = F32(0)
        for k in range(3):
            upper = pl.ds(k * width, upto)
            value = value + dot(low_wide[at, k * width : k * width + upto], core_stack[upper, :])
        row_panel[s, at, :] = value
        out_ref[at, :] = value

    @pl.when(both(prow == 0, pcol > 0))
    def _():
        take_picked(0)
        for chunk in range(tiles):
            row_product(0, chunk)
            if chunk > 0:
                row_flows[0].send(chunk - 1, row_panel.at[0])
        row_flows[0].send(tiles - 1, row_panel.at[0])

    later = both(prow > 0, prow < min(CORES, sections), pcol > 0)

    def land_tops():
        for s in range(sections):

            @pl.when(prow == s)
            def _(s=s):
                pltpu.make_async_copy(
                    tile_ref.at[pl.ds(0, width)], top.at[pl.ds(s * width, width)], local_sem.at[4]
                ).wait()

        for chunk in range(tiles):
            for flow in top_flows:
                flow.pass_on(chunk)
            if chunk == tiles - 2:
                for s in range(sections):
                    pass_picked(s, jnp.logical_not(urgent(s)))

            def cut_top(s, carry, chunk=chunk):
                start = s * width + chunk * step_rows
                at = pl.ds(pl.multiple_of(start, step_rows), step_rows)
                for k, part in enumerate(split3(top[at, :])):
                    top_parts[k, at, :] = part
                return carry

            lax.fori_loop(0, sections, cut_top, 0)

    pl.when(jnp.logical_not(later))(land_tops)

    def settle(block, first_part=0, parts_count=1, size=width):
        def place(i, carry):
            start = i * size
            at = pl.ds(pl.multiple_of(block * width + start, size), size)
            rows = column(start + (block * prow_count + prow) * width, size)
            rows = undo(rows, sections)
            chosen = one_hot(rows, lanes(sections * width))
            value = (
                dot(chosen, top_parts[2]) + dot(chosen, top_parts[1]) + dot(chosen, top_parts[0])
            )
            out_ref[at, :] = jnp.where(rows < F32(sections * width), value, first[at, :])
            return carry

        lax.fori_loop(first_part, first_part + parts_count, place, 0)

    def forwards(s):
        return both(core == s % CORES, prow != s)

    def pass_row(s):
        for chunk in range(tiles):
            row_flows[s].pass_on(chunk)

    def take_row(s):
        @pl.when(jnp.logical_not(forwards(s)))
        def _():
            pass_row(s)

        def cut(i, carry):
            at = pl.ds(pl.multiple_of(i * step_rows, step_rows), step_rows)
            stack(row_stack.at[s], i, row_panel[s, at, :])
            return carry

        lax.fori_loop(0, tiles, cut, 0)

    @pl.when(pcol == 0)
    def _():
        @pl.when(jnp.logical_not(owns_row))
        def _():
            for half in range(2):
                settle(0, half, 1, width // 2)
                produce_first(half * per_block // 2, (half + 1) * per_block // 2)

        for block in range(1, blocks):
            settle(block)
        for s in range(CORES, sections):

            @pl.when(prow == s)
            def _(s=s):
                take_picked(s)

        if sections > 1:

            @pl.when(prow == 0)
            def _():
                pl.semaphore_wait(gate, 1)

        paired = [s for s in range(CORES, sections) if s ^ 1 >= sections]
        for s in paired:

            @pl.when(prow == s ^ 1)
            def _():
                pl.semaphore_wait(gate, 1)

        done = jnp.logical_or(both(prow > 0, prow < CORES), jnp.logical_not(owns_row))
        produce_first(jnp.where(done, per_block, 0), live(0) * per_block)
        for s in paired:

            @pl.when(prow == s)
            def _():
                pl.semaphore_signal(gate, inc=1, device_id=partner, device_id_type=MESH)

    @pl.when(both(pcol > 0, jnp.logical_not(later)))
    def _():
        for block in range(1, blocks):
            settle(block)

        @pl.when(jnp.logical_not(owns_row))
        def _():
            settle(0)

    begin, begin_of, lates, computes, counts = jnp.int32(0), [], [], [], []
    forward_at = []
    for s in range(sections):
        counts.append(live(s) * per_block)
        begin_of.append(begin)
        lates.append(
            [begin + pick_static(pcol, {n: HOP * h for n, h in plan[0].items()}) for plan in plans[s]]
        )
        lag = {n: HOP * farthest(s, n) + (LAG if n != s + 1 else 0) for n in range(pcol_count)}
        slack = jnp.where(x == 0, per_block, 0) if s == 0 else 0
        rest = PATIENCE if s == 0 else 0
        wait = jnp.where(both(prow >= CORES, prow < sections, pcol != 1), rest, 0)
        early = {n: HOP * farthest(s, n) - EARLY[min(s, 1)] for n in range(pcol_count)}
        forward_at.append(begin + pick_static(pcol, early))
        computes.append(begin + pick_static(pcol, lag) + jnp.where(pcol == s + 1, slack, wait))
        if s + 1 < sections:
            begin = begin + HOP * farthest(s, s + 1) + 1 + slack
            begin = begin + jnp.where(prow == s + 1, per_block, 0)
            for n in range(s + 2, pcol_count):
                ahead = HOP * (farthest(s, s + 1) + farthest(s + 1, n) - farthest(s, n))
                assert ahead + 1 >= (LAG if n == s + 2 else 0) + rest

    def inline(s):
        return pcol < 0 if s + 1 == sections else pcol > s

    def compute(s, j):
        last = s + 1 == sections
        skip = 0 if last else counts[s] - counts[s + 1]

        @pl.when(j == 0)
        def _():
            if s == 0:
                for other in range(1, sections):

                    @pl.when(prow == other)
                    def _(other=other):
                        take_picked(other)

            take_row(s)

        if s == 0:

            @pl.when(both(later, j == per_block))
            def _():
                land_tops()
                for block in range(1, blocks):
                    settle(block)

        at = rows_of(s, j)
        value = update(s, at)
        if last:
            out_ref[at, :] = value
            return
        makes = both(pcol == s + 1, j >= skip)

        @pl.when(jnp.logical_not(makes))
        def _():
            out_ref[at, :] = value

        @pl.when(makes)
        def _():
            produce(s + 1, j - skip, value)

        per_tile = per_block // tiles
        for chunk in range(tiles):
            ready = (chunk + 1) * per_tile - 1

            @pl.when(both(prow == s + 1, pcol > s + 1, j == ready))
            def _(chunk=chunk):
                row_product(s + 1, chunk)
                if chunk == tiles - 1:
                    row_flows[s + 1].send(chunk, row_panel.at[s + 1])

            if chunk < tiles - 1:

                @pl.when(both(prow == s + 1, pcol > s + 1, j == ready + 1))
                def _(chunk=chunk):
                    row_flows[s + 1].send(chunk, row_panel.at[s + 1])

    def turn(t, carry):
        for s in range(sections):
            for k in range(2):
                i = t - lates[s][k]

                @pl.when(both(gets[s][k], i >= 0, i < counts[s]))
                def _(s=s, k=k, i=i):
                    for h in range(PARTS):
                        col_copy(s, k, i, h, 0).wait_recv()
                        col_start(s, k, i, h)

            @pl.when(both(inline(s), forwards(s), t == jnp.maximum(forward_at[s], 0)))
            def _(s=s):
                pass_row(s)

            if s > 0:
                i = t - begin_of[s]

                @pl.when(both(pcol == s, i >= 0, i < counts[s]))
                def _(s=s, i=i):
                    start_both(s, i)

            j = t - computes[s]

            @pl.when(both(inline(s), j >= 0, j < counts[s]))
            def _(s=s, j=j):
                compute(s, j)

        return carry

    stop = jnp.int32(0)
    for s in range(sections):
        stop = jnp.maximum(stop, jnp.where(inline(s), computes[s] + counts[s], 0))
        for k in range(2):
            stop = jnp.maximum(stop, jnp.where(gets[s][k], lates[s][k] + counts[s], 0))
        if s > 0:
            stop = jnp.maximum(stop, jnp.where(pcol == s, begin_of[s] + counts[s], 0))
    lax.fori_loop(0, stop, turn, 0)
    last = sections - 1

    @pl.when(both(prow == 0, pcol == 0))
    def _():
        take_picked(0)

    @pl.when(both(pcol > last, jnp.logical_not(inline(last))))
    def _():
        @pl.when(forwards(last))
        def _():
            pass_row(last)

        take_row(last)

    def save(block):
        at = pl.ds(block * width, width)
        return pltpu.make_async_copy(out_ref.at[at], final_ref.at[at], local_sem.at[block])

    for block in range(blocks):

        @pl.when(both(pcol > last, block >= blocks - live(last)))
        def _(block=block):
            at = pl.ds(block * width, width)
            out_ref[at, :] = update(last, at)

        save(block).start()

    for s in range(sections):
        top_flows[s].finish(tiles)

        @pl.when(pcol > s)
        def _(s=s):
            row_flows[s].finish(tiles)

        owner = s // CORES

        @pl.when(core != s % CORES)
        def _(s=s):
            pick_copy(s, 0, 0, partner).wait_send()

        @pl.when(both(core == s % CORES, x != owner))
        def _(s=s):
            pick_copy(s, 0, 1, partner).wait_send()

        for k in range(2):
            for way in range(4):
                for count in (blocks - 1, blocks):

                    @pl.when(both(sends[s][k][way], live(s) == count))
                    def _(s=s, k=k, way=way, count=count):
                        piece = pl.ds(0, count * width // 2)
                        pltpu.make_async_remote_copy(
                            src_ref=col_panel.at[s, piece],
                            dst_ref=col_panel.at[s, piece],
                            send_sem=col_send.at[s, k, way],
                            recv_sem=col_recv.at[s, k, 0],
                            device_id=ways[way][1],
                            device_id_type=MESH,
                        ).wait_send()

    for block in range(blocks):
        save(block).wait()


def on_device(matrix, pivots, lower_inv, upper_inv):
    prow_count = lax.axis_size("prow")
    pcol_count = lax.axis_size("pcol")
    tile = matrix[0, 0]
    rows, width = tile.shape
    sections = pivots.shape[0]
    blocks = rows // width
    assert width == pivots.shape[1] and sections <= prow_count and sections <= pcol_count
    tiles = 3
    relays = blocks * 6
    dma = pltpu.SemaphoreType.DMA
    args = (tile, pivots, lower_inv, upper_inv)
    out = pl.pallas_call(
        functools.partial(factor_kernel, prow_count, pcol_count, sections, width, blocks),
        out_shape=jax.ShapeDtypeStruct(tile.shape, tile.dtype),
        in_specs=[pl.BlockSpec(memory_space=pl.ANY)] * 4,
        out_specs=pl.BlockSpec(memory_space=pl.ANY),
        scratch_shapes=[
            pltpu.VMEM((rows, width), F32),
            pltpu.VMEM((rows, width), F32),
            pltpu.VMEM(pivots.shape, jnp.int32),
            pltpu.VMEM((width, width), F32),
            pltpu.VMEM((width, width), F32),
            pltpu.VMEM((3, rows, width), BF16),
            pltpu.VMEM((sections * width, width), F32),
            pltpu.VMEM((3, sections * width, width), BF16),
            pltpu.VMEM((sections, width, width), F32),
            pltpu.VMEM((sections, 3, width, width), F32),
            pltpu.VMEM((sections, width, width), F32),
            pltpu.VMEM((sections, rows, width), F32),
            pltpu.VMEM((sections, 3 * width, width), BF16),
            pltpu.VMEM((width, 3 * width), BF16),
            pltpu.VMEM((3 * width, width), BF16),
            pltpu.VMEM((3 * width, width), BF16),
            dma((4 + blocks,)),
            dma((sections, 3)),
            dma((sections, tiles)),
            dma((sections, 2)),
            dma((sections, 3)),
            dma((sections, 3)),
            dma((sections, tiles)),
            dma((sections, 2, 4)),
            dma((sections, 2, relays * PARTS)),
            pltpu.SemaphoreType.REGULAR,
        ],
        compiler_params=pltpu.CompilerParams(
            collective_id=0, has_side_effects=True, vmem_limit_bytes=40 * 1024 * 1024
        ),
    )(*[pltpu.with_memory_space_constraint(v, pltpu.HBM) for v in args])
    return out[None, None]


def solution(mesh):
    return jax.shard_map(
        on_device,
        mesh=mesh,
        in_specs=(P("prow", "pcol", None, None), P(), P(), P()),
        out_specs=P("prow", "pcol", None, None),
        check_vma=False,
    )
```

```python
import functools

import jax
import jax.numpy as jnp
from jax import lax
from jax.experimental import pallas as pl
from jax.experimental.pallas import tpu as pltpu
from jax.sharding import PartitionSpec as P

MESH = pl.DeviceIdType.MESH
CORES = 2
F32 = jnp.float32
BF16 = jnp.bfloat16
HOP = 3
EARLY = (4, 0)
PARTS = 1
PATIENCE = 4
LAG = 2


def grid_width(count):
    width = 1
    while (2 * width) * (2 * width) <= count:
        width *= 2
    return width if count % width == 0 else 1


def both(*conds):
    out = conds[0]
    for cond in conds[1:]:
        out = jnp.logical_and(out, cond)
    return out


def entry_barrier(neighbours):
    barrier = pltpu.get_barrier_semaphore()
    total = jnp.int32(0)
    for cond, device in neighbours:
        total = total + jnp.where(cond, 1, 0).astype(jnp.int32)

        @pl.when(cond)
        def _(device=device):
            pl.semaphore_signal(barrier, inc=1, device_id=device, device_id_type=MESH)

    pl.semaphore_wait(barrier, total)


def line_ways(prow, prow_count):
    x, core = prow // CORES, prow % CORES
    chips = prow_count // CORES
    return [
        (x + 1 < chips, {"prow": prow + CORES}),
        (x > 0, {"prow": prow - CORES}),
        (prow >= 0, {"prow": x * CORES + (CORES - 1 - core)}),
    ]


def line_sends(prow, prow_count, source):
    x, core = prow // CORES, prow % CORES
    ways = line_ways(prow, prow_count)
    sx, sc = source // CORES, source % CORES
    return [
        (both(ways[0][0], core == sc, x >= sx), ways[0][1]),
        (both(ways[1][0], core == sc, x <= sx), ways[1][1]),
        (core == sc, ways[2][1]),
    ]


def grid_ways(pcol, pcol_count):
    width = grid_width(pcol_count)
    height = pcol_count // width
    z, y = pcol // width, pcol % width
    return [
        (z + 1 < height, {"pcol": pcol + width}),
        (z > 0, {"pcol": pcol - width}),
        (y + 1 < width, {"pcol": pcol + 1}),
        (y > 0, {"pcol": pcol - 1}),
    ]


def tree_plan(pcol_count, source, first_axis):
    width = grid_width(pcol_count)
    extent = (pcol_count // width, width)
    src = (source // width, source % width)
    a, b = first_axis, 1 - first_axis
    near = src[a] + 1 if src[a] + 1 < extent[a] else src[a] - 1

    def toward(at, goal):
        return at + (goal > at) - (goal < at)

    parent = {}
    for node in range(pcol_count):
        pos = [node // width, node % width]
        if node == source:
            continue
        if pos[b] == src[b]:
            pos[a] = toward(pos[a], src[a])
        elif pos[a] != src[a] or extent[a] == 1:
            pos[b] = toward(pos[b], src[b])
        else:
            pos[a] = near
        parent[node] = pos[0] * width + pos[1]
    hops, used = {source: 0}, set()
    for node in range(pcol_count):
        path = [node]
        while path[-1] != source:
            path.append(parent[path[-1]])
        hops[node] = len(path) - 1
        if node > source:
            used.update(path)
    steps = (width, -width, 1, -1)
    senders = [
        [parent[c] for c in used if c != source and c - parent[c] == step]
        if step not in steps[:way] else []
        for way, step in enumerate(steps)
    ]
    return hops, used - {source}, senders


def pick_static(index, table):
    out = jnp.int32(0)
    for key, value in table.items():
        out = jnp.where(index == key, value, out)
    return out


def among(index, members):
    mask = sum(1 << member for member in set(members))
    return (lax.shift_right_logical(jnp.int32(mask), index) & 1) == 1


class Flow:
    def __init__(self, mine, start_ref, land_ref, sends, send_sem, recv_sem, rows):
        self.mine, self.start_ref, self.land_ref = mine, start_ref, land_ref
        self.sends, self.send_sem, self.recv_sem, self.rows = sends, send_sem, recv_sem, rows

    def copy(self, chunk, way, ref):
        piece = pl.ds(chunk * self.rows, self.rows)
        return pltpu.make_async_remote_copy(
            src_ref=ref.at[piece],
            dst_ref=self.land_ref.at[piece],
            send_sem=self.send_sem.at[way],
            recv_sem=self.recv_sem.at[chunk],
            device_id=self.sends[way][1],
            device_id_type=MESH,
        )

    def send(self, chunk, ref):
        for way, (cond, _device) in enumerate(self.sends):

            @pl.when(cond)
            def _(way=way):
                self.copy(chunk, way, ref).start()

    def pass_on(self, chunk):
        @pl.when(jnp.logical_not(self.mine))
        def _():
            self.copy(chunk, 0, self.land_ref).wait_recv()
            self.send(chunk, self.land_ref)

    def finish(self, count):
        piece = pl.ds(0, count * self.rows)
        for way, (cond, device) in enumerate(self.sends):

            @pl.when(cond)
            def _(way=way, device=device):
                pltpu.make_async_remote_copy(
                    src_ref=self.land_ref.at[piece],
                    dst_ref=self.land_ref.at[piece],
                    send_sem=self.send_sem.at[way],
                    recv_sem=self.recv_sem.at[0],
                    device_id=device,
                    device_id_type=MESH,
                ).wait_send()


def split2(value):
    high = value.astype(BF16)
    low = (value - high.astype(F32)).astype(BF16)
    return high, low


def split3(value):
    high = value.astype(BF16)
    rest = value - high.astype(F32)
    middle = rest.astype(BF16)
    low = (rest - middle.astype(F32)).astype(BF16)
    return high, middle, low


def wide(value):
    high, low = split2(value)
    return jnp.concatenate([high, high, low], axis=1)


def dot(left, right):
    return jnp.dot(left, right, preferred_element_type=F32)


def factor_kernel(
    prow_count, pcol_count, sections, width, blocks,
    tile_ref, pivots_ref, lower_ref, upper_ref, final_ref,
    out_ref, first, pivot, low_in, up_in, parts, top, top_parts, picked, picked_in,
    row_panel, col_panel, row_stack, low_wide, up_stack, core_stack,
    local_sem, top_send, top_recv, pick_send, pick_recv,
    row_send, row_recv, col_send, col_recv, gate,
):
    prow = lax.axis_index("prow")
    pcol = lax.axis_index("pcol")
    x, core = prow // CORES, prow % CORES
    chips = prow_count // CORES
    step_rows = width // 3
    tiles = width // step_rows
    relay_rows = PARTS * col_panel.shape[1] // (2 * col_recv.shape[2])
    span = 2 * relay_rows
    per_block = width // span

    load_tile = pltpu.make_async_copy(tile_ref, first, local_sem.at[0])
    load_pivots = pltpu.make_async_copy(pivots_ref, pivot, local_sem.at[1])
    load_pivots.start()
    load_tile.start()
    owns_row = prow < sections
    owns_col = pcol < sections

    @pl.when(owns_row)
    def _():
        pltpu.make_async_copy(lower_ref.at[prow], low_in, local_sem.at[2]).start()

    @pl.when(owns_col)
    def _():
        pltpu.make_async_copy(upper_ref.at[pcol], up_in, local_sem.at[3]).start()

    top_flows = [
        Flow(
            prow == s, tile_ref, top.at[pl.ds(s * width, width)],
            line_sends(prow, prow_count, s), top_send.at[s], top_recv.at[s], step_rows,
        )
        for s in range(sections)
    ]
    row_flows = [
        Flow(
            prow == s, row_panel.at[s], row_panel.at[s],
            line_sends(prow, prow_count, s), row_send.at[s], row_recv.at[s], step_rows,
        )
        for s in range(sections)
    ]

    entry_barrier(line_ways(prow, prow_count) + grid_ways(pcol, pcol_count))

    def waits_for_picks(s):
        return prow >= 0 if s >= CORES else prow < 0

    for s in range(sections):

        @pl.when(prow == s)
        def _(s=s):
            for chunk in range(tiles - 1):
                top_flows[s].send(chunk, tile_ref)

            @pl.when(jnp.logical_not(waits_for_picks(s)))
            def _():
                top_flows[s].send(tiles - 1, tile_ref)

            pltpu.make_async_copy(
                tile_ref.at[pl.ds(0, width)], top.at[pl.ds(s * width, width)], local_sem.at[4]
            ).start()

    def lanes(count):
        return lax.broadcasted_iota(jnp.int32, (1, count), 1).astype(F32)

    def column(start, rows=step_rows):
        ids = lax.broadcasted_iota(jnp.int32, (rows, 1), 0)
        return (ids + start).astype(F32)

    def pivot_row(s):
        return pivot[pl.ds(s, 1), :].astype(F32)

    def undo(rows, upto):
        for s in reversed(range(upto)):
            listed = pivot_row(s)
            shift = lanes(width) + F32(s * width) - listed
            moved = jnp.where(rows == listed, shift, F32(0))
            rows = rows + jnp.sum(moved, axis=1, keepdims=True)
        return rows

    def one_hot(rows, ids):
        return jnp.where(rows == ids, F32(1), F32(0)).astype(BF16)

    load_pivots.wait()
    load_tile.wait()

    def cut_tile(i, carry):
        at = pl.ds(pl.multiple_of(i * step_rows, step_rows), step_rows)
        for k, part in enumerate(split3(first[at, :])):
            parts[k, at, :] = part
        return carry

    lax.fori_loop(0, tiles * blocks, cut_tile, 0)

    def pick_copy(s, slot, where, device):
        return pltpu.make_async_remote_copy(
            src_ref=picked.at[s],
            dst_ref=picked_in.at[s, slot],
            send_sem=pick_send.at[s, where],
            recv_sem=pick_recv.at[s, slot],
            device_id=device,
            device_id_type=MESH,
        )

    partner = {"prow": x * CORES + (CORES - 1 - core)}
    held_ids = jnp.concatenate(
        [
            lanes(width) + ((block * prow_count + prow) * width).astype(F32)
            for block in range(blocks)
        ],
        axis=1,
    )
    def pick_rows(s):
        def pick(i, carry):
            start = i * width
            at = pl.ds(pl.multiple_of(start, width), width)
            rows = jnp.sum(
                jnp.where(column(start, width) == lanes(width), pivot_row(s), F32(0)),
                axis=1, keepdims=True,
            )
            chosen = one_hot(undo(rows, s), held_ids)
            picked[s, at, :] = (
                dot(chosen, parts[2]) + dot(chosen, parts[1]) + dot(chosen, parts[0])
            )
            return carry

        lax.fori_loop(0, width // width, pick, 0)

        @pl.when(core != s % CORES)
        def _():
            pick_copy(s, 0, 0, partner).start()

    def add_in(s, slot):
        pick_copy(s, slot, 1, partner).wait_recv()

        def add(i, carry):
            at = pl.ds(pl.multiple_of(i * step_rows, step_rows), step_rows)
            picked[s, at, :] += picked_in[s, slot, at, :]
            return carry

        lax.fori_loop(0, tiles, add, 0)

    def pass_picked(s, when):
        owner = s // CORES

        @pl.when(both(core == s % CORES, x != owner, when))
        def _():
            add_in(s, 0)

            @pl.when(both(x < owner, x > 0))
            def _():
                add_in(s, 1)

            @pl.when(both(x > owner, x < chips - 1))
            def _():
                add_in(s, 2)

            @pl.when(x < owner)
            def _():
                pick_copy(s, 1, 1, {"prow": prow + CORES}).start()

            @pl.when(x > owner)
            def _():
                pick_copy(s, 2, 1, {"prow": prow - CORES}).start()

    def urgent(s):
        return pcol > 0 if s == 0 else pcol == 0

    def pick_all(order):
        for s in order:
            pick_rows(s)
            pass_picked(s, urgent(s))

    @pl.when(pcol == 0)
    def _():
        pick_all([*range(1, sections), 0])

    @pl.when(pcol > 0)
    def _():
        pick_all([*range(sections)])

    for s in range(sections):

        @pl.when(both(prow == s, waits_for_picks(s)))
        def _(s=s):
            top_flows[s].send(tiles - 1, tile_ref)


    @pl.when(owns_row)
    def _():
        pltpu.make_async_copy(lower_ref.at[prow], low_in, local_sem.at[2]).wait()

        def prepare(i, carry):
            start = i * step_rows
            at = pl.ds(pl.multiple_of(start, step_rows), step_rows)
            below = column(start) > lanes(width)
            same = column(start) == lanes(width)
            unit = jnp.where(below, low_in[at, :], jnp.where(same, F32(1), F32(0)))
            low_wide[at, :] = wide(unit)
            return carry

        lax.fori_loop(0, tiles, prepare, 0)

    def stack(ref, i, value):
        high, low = split2(value)
        start = i * step_rows
        for k, part in enumerate((high, low, high)):
            at = pl.ds(pl.multiple_of(k * width + start, step_rows), step_rows)
            ref[at, :] = part

    @pl.when(owns_col)
    def _():
        pltpu.make_async_copy(upper_ref.at[pcol], up_in, local_sem.at[3]).wait()

        def prepare(i, carry):
            start = i * step_rows
            at = pl.ds(pl.multiple_of(start, step_rows), step_rows)
            kept = jnp.where(column(start) <= lanes(width), up_in[at, :], F32(0))
            stack(up_stack, i, kept)
            return carry

        lax.fori_loop(0, tiles, prepare, 0)

    def take_picked(s):
        owner = s // CORES
        add_in(s, 0)
        slots = [1] * (owner > 0) + [2] * (owner < chips - 1)
        for slot in slots[:-1]:
            add_in(s, slot)
        for slot in slots[-1:]:
            pick_copy(s, slot, 1, partner).wait_recv()

        def put(i, carry):
            at = pl.ds(pl.multiple_of(i * step_rows, step_rows), step_rows)
            value = picked[s, at, :]
            for slot in slots[-1:]:
                value = value + picked_in[s, slot, at, :]
            out_ref[at, :] = value
            return carry

        lax.fori_loop(0, tiles, put, 0)

    ways = grid_ways(pcol, pcol_count)
    plans = [[tree_plan(pcol_count, s, k) for k in range(2)] for s in range(sections)]
    sends = [[[among(pcol, who) for who in plan[2]] for plan in pair] for pair in plans]
    gets = [[among(pcol, plan[1]) for plan in pair] for pair in plans]

    def farthest(s, node):
        return max(plan[0][node] for plan in plans[s])

    def live(s):
        return jnp.where(prow > s, blocks, blocks - 1)

    def place_of(s, i):
        turn = lax.div(i, per_block)
        block = blocks - live(s) + turn
        return block * width + (i - turn * per_block) * span

    part_rows = relay_rows // PARTS

    def col_copy(s, k, i, h, way):
        start = place_of(s, i) + k * relay_rows + h * part_rows
        piece = pl.ds(pl.multiple_of(start, part_rows), part_rows)
        return pltpu.make_async_remote_copy(
            src_ref=col_panel.at[s, piece],
            dst_ref=col_panel.at[s, piece],
            send_sem=col_send.at[s, k, way],
            recv_sem=col_recv.at[s, k, i * PARTS + h],
            device_id=ways[way][1],
            device_id_type=MESH,
        )

    def col_start(s, k, i, h):
        for way in range(4):

            @pl.when(sends[s][k][way])
            def _(way=way):
                col_copy(s, k, i, h, way).start()

    def update(s, at):
        return out_ref[at, :] - dot(wide(col_panel[s, at, :]), row_stack[s])

    def rows_of(s, i):
        return pl.ds(pl.multiple_of(place_of(s, i), span), span)

    def produce(s, i, value):
        at = rows_of(s, i)
        value = dot(wide(value), up_stack[...])
        col_panel[s, at, :] = value
        out_ref[at, :] = value

    def start_both(s, i):
        for h in range(PARTS):
            for k in range(2):
                col_start(s, k, i, h)

    def produce_first(start, stop):
        def body(i, carry):
            produce(0, i, out_ref[rows_of(0, i), :])

            @pl.when(i > start)
            def _():
                start_both(0, i - 1)

            return carry

        lax.fori_loop(start, stop, body, 0)
        start_both(0, stop - 1)

    for s in range(1, min(CORES, sections)):

        @pl.when(both(pcol == 0, prow == s))
        def _(s=s):
            take_picked(s)
            produce_first(0, per_block)
            pl.semaphore_signal(gate, inc=1, device_id=partner, device_id_type=MESH)

    def row_product(s, chunk):
        at = pl.ds(chunk * step_rows, step_rows)
        stack(core_stack, chunk, out_ref[at, :])
        upto = (chunk + 1) * step_rows
        value = F32(0)
        for k in range(3):
            upper = pl.ds(k * width, upto)
            value = value + dot(low_wide[at, k * width : k * width + upto], core_stack[upper, :])
        row_panel[s, at, :] = value
        out_ref[at, :] = value

    @pl.when(both(prow == 0, pcol > 0))
    def _():
        take_picked(0)
        for chunk in range(tiles):
            row_product(0, chunk)
            if chunk > 0:
                row_flows[0].send(chunk - 1, row_panel.at[0])
        row_flows[0].send(tiles - 1, row_panel.at[0])

    later = both(prow > 0, prow < min(CORES, sections), pcol > 0)

    def land_tops():
        for s in range(sections):

            @pl.when(prow == s)
            def _(s=s):
                pltpu.make_async_copy(
                    tile_ref.at[pl.ds(0, width)], top.at[pl.ds(s * width, width)], local_sem.at[4]
                ).wait()

        for chunk in range(tiles):
            for flow in top_flows:
                flow.pass_on(chunk)
            if chunk == tiles - 2:
                for s in range(sections):
                    pass_picked(s, jnp.logical_not(urgent(s)))

            def cut_top(s, carry, chunk=chunk):
                start = s * width + chunk * step_rows
                at = pl.ds(pl.multiple_of(start, step_rows), step_rows)
                for k, part in enumerate(split3(top[at, :])):
                    top_parts[k, at, :] = part
                return carry

            lax.fori_loop(0, sections, cut_top, 0)

    pl.when(jnp.logical_not(later))(land_tops)

    def settle(block, first_part=0, parts_count=1, size=width):
        def place(i, carry):
            start = i * size
            at = pl.ds(pl.multiple_of(block * width + start, size), size)
            rows = column(start + (block * prow_count + prow) * width, size)
            rows = undo(rows, sections)
            chosen = one_hot(rows, lanes(sections * width))
            value = (
                dot(chosen, top_parts[2]) + dot(chosen, top_parts[1]) + dot(chosen, top_parts[0])
            )
            out_ref[at, :] = jnp.where(rows < F32(sections * width), value, first[at, :])
            return carry

        lax.fori_loop(first_part, first_part + parts_count, place, 0)

    def forwards(s):
        return both(core == s % CORES, prow != s)

    def pass_row(s):
        for chunk in range(tiles):
            row_flows[s].pass_on(chunk)

    def take_row(s):
        @pl.when(jnp.logical_not(forwards(s)))
        def _():
            pass_row(s)

        def cut(i, carry):
            at = pl.ds(pl.multiple_of(i * step_rows, step_rows), step_rows)
            stack(row_stack.at[s], i, row_panel[s, at, :])
            return carry

        lax.fori_loop(0, tiles, cut, 0)

    @pl.when(pcol == 0)
    def _():
        @pl.when(jnp.logical_not(owns_row))
        def _():
            for half in range(2):
                settle(0, half, 1, width // 2)
                produce_first(half * per_block // 2, (half + 1) * per_block // 2)

        for block in range(1, blocks):
            settle(block)
        for s in range(CORES, sections):

            @pl.when(prow == s)
            def _(s=s):
                take_picked(s)

        if sections > 1:

            @pl.when(prow == 0)
            def _():
                pl.semaphore_wait(gate, 1)

        paired = [s for s in range(CORES, sections) if s ^ 1 >= sections]
        for s in paired:

            @pl.when(prow == s ^ 1)
            def _():
                pl.semaphore_wait(gate, 1)

        for s in paired:

            @pl.when(prow == s)
            def _():
                produce_first(0, per_block + per_block // 2)
                pl.semaphore_signal(gate, inc=1, device_id=partner, device_id_type=MESH)

        done = jnp.where(both(prow > 0, prow < CORES) | jnp.logical_not(owns_row), per_block, 0)
        for s in paired:
            done = jnp.where(prow == s, per_block + per_block // 2, done)
        produce_first(done, live(0) * per_block)

    @pl.when(both(pcol > 0, jnp.logical_not(later)))
    def _():
        for block in range(1, blocks):
            settle(block)

        @pl.when(jnp.logical_not(owns_row))
        def _():
            settle(0)

    begin, begin_of, lates, computes, counts = jnp.int32(0), [], [], [], []
    forward_at = []
    for s in range(sections):
        counts.append(live(s) * per_block)
        begin_of.append(begin)
        lates.append(
            [begin + pick_static(pcol, {n: HOP * h for n, h in plan[0].items()}) for plan in plans[s]]
        )
        lag = {n: HOP * farthest(s, n) + (LAG if n != s + 1 else 0) for n in range(pcol_count)}
        slack = jnp.where(x == 0, per_block, 0) if s == 0 else 0
        rest = PATIENCE if s == 0 else 0
        wait = jnp.where(both(prow >= CORES, prow < sections, pcol != 1), rest, 0)
        early = {n: HOP * farthest(s, n) - EARLY[min(s, 1)] for n in range(pcol_count)}
        forward_at.append(begin + pick_static(pcol, early))
        computes.append(begin + pick_static(pcol, lag) + jnp.where(pcol == s + 1, slack, wait))
        if s + 1 < sections:
            begin = begin + HOP * farthest(s, s + 1) + 1 + slack
            begin = begin + jnp.where(prow == s + 1, per_block, 0)
            for n in range(s + 2, pcol_count):
                ahead = HOP * (farthest(s, s + 1) + farthest(s + 1, n) - farthest(s, n))
                assert ahead + 1 >= (LAG if n == s + 2 else 0) + rest

    def inline(s):
        return pcol < 0 if s + 1 == sections else pcol > s

    def compute(s, j):
        last = s + 1 == sections
        skip = 0 if last else counts[s] - counts[s + 1]

        @pl.when(j == 0)
        def _():
            if s == 0:
                for other in range(1, sections):

                    @pl.when(prow == other)
                    def _(other=other):
                        take_picked(other)

            take_row(s)

        if s == 0:

            @pl.when(both(later, j == per_block))
            def _():
                land_tops()
                for block in range(1, blocks):
                    settle(block)

        at = rows_of(s, j)
        value = update(s, at)
        if last:
            out_ref[at, :] = value
            return
        makes = both(pcol == s + 1, j >= skip)

        @pl.when(jnp.logical_not(makes))
        def _():
            out_ref[at, :] = value

        @pl.when(makes)
        def _():
            produce(s + 1, j - skip, value)

        per_tile = per_block // tiles
        for chunk in range(tiles):
            ready = (chunk + 1) * per_tile - 1

            @pl.when(both(prow == s + 1, pcol > s + 1, j == ready))
            def _(chunk=chunk):
                row_product(s + 1, chunk)
                if chunk == tiles - 1:
                    row_flows[s + 1].send(chunk, row_panel.at[s + 1])

            if chunk < tiles - 1:

                @pl.when(both(prow == s + 1, pcol > s + 1, j == ready + 1))
                def _(chunk=chunk):
                    row_flows[s + 1].send(chunk, row_panel.at[s + 1])

    def turn(t, carry):
        for s in range(sections):
            for k in range(2):
                i = t - lates[s][k]

                @pl.when(both(gets[s][k], i >= 0, i < counts[s]))
                def _(s=s, k=k, i=i):
                    for h in range(PARTS):
                        col_copy(s, k, i, h, 0).wait_recv()
                        col_start(s, k, i, h)

            @pl.when(both(inline(s), forwards(s), t == jnp.maximum(forward_at[s], 0)))
            def _(s=s):
                pass_row(s)

            if s > 0:
                i = t - begin_of[s]

                @pl.when(both(pcol == s, i >= 0, i < counts[s]))
                def _(s=s, i=i):
                    start_both(s, i)

            j = t - computes[s]

            @pl.when(both(inline(s), j >= 0, j < counts[s]))
            def _(s=s, j=j):
                compute(s, j)

        return carry

    stop = jnp.int32(0)
    for s in range(sections):
        stop = jnp.maximum(stop, jnp.where(inline(s), computes[s] + counts[s], 0))
        for k in range(2):
            stop = jnp.maximum(stop, jnp.where(gets[s][k], lates[s][k] + counts[s], 0))
        if s > 0:
            stop = jnp.maximum(stop, jnp.where(pcol == s, begin_of[s] + counts[s], 0))
    lax.fori_loop(0, stop, turn, 0)
    last = sections - 1

    @pl.when(both(prow == 0, pcol == 0))
    def _():
        take_picked(0)

    @pl.when(both(pcol > last, jnp.logical_not(inline(last))))
    def _():
        @pl.when(forwards(last))
        def _():
            pass_row(last)

        take_row(last)

    def save(block):
        at = pl.ds(block * width, width)
        return pltpu.make_async_copy(out_ref.at[at], final_ref.at[at], local_sem.at[block])

    for block in range(blocks):

        @pl.when(both(pcol > last, block >= blocks - live(last)))
        def _(block=block):
            at = pl.ds(block * width, width)
            out_ref[at, :] = update(last, at)

        save(block).start()

    for s in range(sections):
        top_flows[s].finish(tiles)

        @pl.when(pcol > s)
        def _(s=s):
            row_flows[s].finish(tiles)

        owner = s // CORES

        @pl.when(core != s % CORES)
        def _(s=s):
            pick_copy(s, 0, 0, partner).wait_send()

        @pl.when(both(core == s % CORES, x != owner))
        def _(s=s):
            pick_copy(s, 0, 1, partner).wait_send()

        for k in range(2):
            for way in range(4):
                for count in (blocks - 1, blocks):

                    @pl.when(both(sends[s][k][way], live(s) == count))
                    def _(s=s, k=k, way=way, count=count):
                        piece = pl.ds(0, count * width // 2)
                        pltpu.make_async_remote_copy(
                            src_ref=col_panel.at[s, piece],
                            dst_ref=col_panel.at[s, piece],
                            send_sem=col_send.at[s, k, way],
                            recv_sem=col_recv.at[s, k, 0],
                            device_id=ways[way][1],
                            device_id_type=MESH,
                        ).wait_send()

    for block in range(blocks):
        save(block).wait()


def on_device(matrix, pivots, lower_inv, upper_inv):
    prow_count = lax.axis_size("prow")
    pcol_count = lax.axis_size("pcol")
    tile = matrix[0, 0]
    rows, width = tile.shape
    sections = pivots.shape[0]
    blocks = rows // width
    assert width == pivots.shape[1] and sections <= prow_count and sections <= pcol_count
    tiles = 3
    relays = blocks * 6
    dma = pltpu.SemaphoreType.DMA
    args = (tile, pivots, lower_inv, upper_inv)
    out = pl.pallas_call(
        functools.partial(factor_kernel, prow_count, pcol_count, sections, width, blocks),
        out_shape=jax.ShapeDtypeStruct(tile.shape, tile.dtype),
        in_specs=[pl.BlockSpec(memory_space=pl.ANY)] * 4,
        out_specs=pl.BlockSpec(memory_space=pl.ANY),
        scratch_shapes=[
            pltpu.VMEM((rows, width), F32),
            pltpu.VMEM((rows, width), F32),
            pltpu.VMEM(pivots.shape, jnp.int32),
            pltpu.VMEM((width, width), F32),
            pltpu.VMEM((width, width), F32),
            pltpu.VMEM((3, rows, width), BF16),
            pltpu.VMEM((sections * width, width), F32),
            pltpu.VMEM((3, sections * width, width), BF16),
            pltpu.VMEM((sections, width, width), F32),
            pltpu.VMEM((sections, 3, width, width), F32),
            pltpu.VMEM((sections, width, width), F32),
            pltpu.VMEM((sections, rows, width), F32),
            pltpu.VMEM((sections, 3 * width, width), BF16),
            pltpu.VMEM((width, 3 * width), BF16),
            pltpu.VMEM((3 * width, width), BF16),
            pltpu.VMEM((3 * width, width), BF16),
            dma((4 + blocks,)),
            dma((sections, 3)),
            dma((sections, tiles)),
            dma((sections, 2)),
            dma((sections, 3)),
            dma((sections, 3)),
            dma((sections, tiles)),
            dma((sections, 2, 4)),
            dma((sections, 2, relays * PARTS)),
            pltpu.SemaphoreType.REGULAR,
        ],
        compiler_params=pltpu.CompilerParams(
            collective_id=0, has_side_effects=True, vmem_limit_bytes=40 * 1024 * 1024
        ),
    )(*[pltpu.with_memory_space_constraint(v, pltpu.HBM) for v in args])
    return out[None, None]


def solution(mesh):
    return jax.shard_map(
        on_device,
        mesh=mesh,
        in_specs=(P("prow", "pcol", None, None), P(), P(), P()),
        out_specs=P("prow", "pcol", None, None),
        check_vma=False,
    )
```

```python
import functools

import jax
import jax.numpy as jnp
from jax import lax
from jax.experimental import pallas as pl
from jax.experimental.pallas import tpu as pltpu
from jax.sharding import PartitionSpec as P

MESH = pl.DeviceIdType.MESH
CORES = 2
F32 = jnp.float32
BF16 = jnp.bfloat16
HOP = 3
EARLY = (4, 0)
PARTS = 1
PATIENCE = 4
LAG = 2


def grid_width(count):
    width = 1
    while (2 * width) * (2 * width) <= count:
        width *= 2
    return width if count % width == 0 else 1


def both(*conds):
    out = conds[0]
    for cond in conds[1:]:
        out = jnp.logical_and(out, cond)
    return out


def entry_barrier(neighbours):
    barrier = pltpu.get_barrier_semaphore()
    total = jnp.int32(0)
    for cond, device in neighbours:
        total = total + jnp.where(cond, 1, 0).astype(jnp.int32)

        @pl.when(cond)
        def _(device=device):
            pl.semaphore_signal(barrier, inc=1, device_id=device, device_id_type=MESH)

    pl.semaphore_wait(barrier, total)


def line_ways(prow, prow_count):
    x, core = prow // CORES, prow % CORES
    chips = prow_count // CORES
    return [
        (x + 1 < chips, {"prow": prow + CORES}),
        (x > 0, {"prow": prow - CORES}),
        (prow >= 0, {"prow": x * CORES + (CORES - 1 - core)}),
    ]


def line_sends(prow, prow_count, source):
    x, core = prow // CORES, prow % CORES
    ways = line_ways(prow, prow_count)
    sx, sc = source // CORES, source % CORES
    return [
        (both(ways[0][0], core == sc, x >= sx), ways[0][1]),
        (both(ways[1][0], core == sc, x <= sx), ways[1][1]),
        (core == sc, ways[2][1]),
    ]


def grid_ways(pcol, pcol_count):
    width = grid_width(pcol_count)
    height = pcol_count // width
    z, y = pcol // width, pcol % width
    return [
        (z + 1 < height, {"pcol": pcol + width}),
        (z > 0, {"pcol": pcol - width}),
        (y + 1 < width, {"pcol": pcol + 1}),
        (y > 0, {"pcol": pcol - 1}),
    ]


def tree_plan(pcol_count, source, first_axis):
    width = grid_width(pcol_count)
    extent = (pcol_count // width, width)
    src = (source // width, source % width)
    a, b = first_axis, 1 - first_axis
    near = src[a] + 1 if src[a] + 1 < extent[a] else src[a] - 1

    def toward(at, goal):
        return at + (goal > at) - (goal < at)

    parent = {}
    for node in range(pcol_count):
        pos = [node // width, node % width]
        if node == source:
            continue
        if pos[b] == src[b]:
            pos[a] = toward(pos[a], src[a])
        elif pos[a] != src[a] or extent[a] == 1:
            pos[b] = toward(pos[b], src[b])
        else:
            pos[a] = near
        parent[node] = pos[0] * width + pos[1]
    hops, used = {source: 0}, set()
    for node in range(pcol_count):
        path = [node]
        while path[-1] != source:
            path.append(parent[path[-1]])
        hops[node] = len(path) - 1
        if node > source:
            used.update(path)
    steps = (width, -width, 1, -1)
    senders = [
        [parent[c] for c in used if c != source and c - parent[c] == step]
        if step not in steps[:way] else []
        for way, step in enumerate(steps)
    ]
    return hops, used - {source}, senders


def pick_static(index, table):
    out = jnp.int32(0)
    for key, value in table.items():
        out = jnp.where(index == key, value, out)
    return out


def among(index, members):
    mask = sum(1 << member for member in set(members))
    return (lax.shift_right_logical(jnp.int32(mask), index) & 1) == 1


class Flow:
    def __init__(self, mine, start_ref, land_ref, sends, send_sem, recv_sem, rows):
        self.mine, self.start_ref, self.land_ref = mine, start_ref, land_ref
        self.sends, self.send_sem, self.recv_sem, self.rows = sends, send_sem, recv_sem, rows

    def copy(self, chunk, way, ref):
        piece = pl.ds(chunk * self.rows, self.rows)
        return pltpu.make_async_remote_copy(
            src_ref=ref.at[piece],
            dst_ref=self.land_ref.at[piece],
            send_sem=self.send_sem.at[way],
            recv_sem=self.recv_sem.at[chunk],
            device_id=self.sends[way][1],
            device_id_type=MESH,
        )

    def send(self, chunk, ref):
        for way, (cond, _device) in enumerate(self.sends):

            @pl.when(cond)
            def _(way=way):
                self.copy(chunk, way, ref).start()

    def pass_on(self, chunk):
        @pl.when(jnp.logical_not(self.mine))
        def _():
            self.copy(chunk, 0, self.land_ref).wait_recv()
            self.send(chunk, self.land_ref)

    def finish(self, count):
        piece = pl.ds(0, count * self.rows)
        for way, (cond, device) in enumerate(self.sends):

            @pl.when(cond)
            def _(way=way, device=device):
                pltpu.make_async_remote_copy(
                    src_ref=self.land_ref.at[piece],
                    dst_ref=self.land_ref.at[piece],
                    send_sem=self.send_sem.at[way],
                    recv_sem=self.recv_sem.at[0],
                    device_id=device,
                    device_id_type=MESH,
                ).wait_send()


def split2(value):
    high = value.astype(BF16)
    low = (value - high.astype(F32)).astype(BF16)
    return high, low


def split3(value):
    high = value.astype(BF16)
    rest = value - high.astype(F32)
    middle = rest.astype(BF16)
    low = (rest - middle.astype(F32)).astype(BF16)
    return high, middle, low


def wide(value):
    high, low = split2(value)
    return jnp.concatenate([high, high, low], axis=1)


def dot(left, right):
    return jnp.dot(left, right, preferred_element_type=F32)


def factor_kernel(
    prow_count, pcol_count, sections, width, blocks,
    tile_ref, pivots_ref, lower_ref, upper_ref, final_ref,
    out_ref, first, pivot, low_in, up_in, parts, top, top_parts, picked, picked_in,
    row_panel, col_panel, row_stack, low_wide, up_stack, core_stack,
    local_sem, top_send, top_recv, pick_send, pick_recv,
    row_send, row_recv, col_send, col_recv, gate,
):
    prow = lax.axis_index("prow")
    pcol = lax.axis_index("pcol")
    x, core = prow // CORES, prow % CORES
    chips = prow_count // CORES
    step_rows = width // 3
    tiles = width // step_rows
    relay_rows = PARTS * col_panel.shape[1] // (2 * col_recv.shape[2])
    span = 2 * relay_rows
    per_block = width // span

    load_tile = pltpu.make_async_copy(tile_ref, first, local_sem.at[0])
    load_pivots = pltpu.make_async_copy(pivots_ref, pivot, local_sem.at[1])
    load_pivots.start()
    load_tile.start()
    owns_row = prow < sections
    owns_col = pcol < sections

    @pl.when(owns_row)
    def _():
        pltpu.make_async_copy(lower_ref.at[prow], low_in, local_sem.at[2]).start()

    @pl.when(owns_col)
    def _():
        pltpu.make_async_copy(upper_ref.at[pcol], up_in, local_sem.at[3]).start()

    top_flows = [
        Flow(
            prow == s, tile_ref, top.at[pl.ds(s * width, width)],
            line_sends(prow, prow_count, s), top_send.at[s], top_recv.at[s], step_rows,
        )
        for s in range(sections)
    ]
    row_flows = [
        Flow(
            prow == s, row_panel.at[s], row_panel.at[s],
            line_sends(prow, prow_count, s), row_send.at[s], row_recv.at[s], step_rows,
        )
        for s in range(sections)
    ]

    entry_barrier(line_ways(prow, prow_count) + grid_ways(pcol, pcol_count))

    def waits_for_picks(s):
        return prow >= 0 if s >= CORES else prow < 0

    for s in range(sections):

        @pl.when(prow == s)
        def _(s=s):
            for chunk in range(tiles - 1):
                top_flows[s].send(chunk, tile_ref)

            @pl.when(jnp.logical_not(waits_for_picks(s)))
            def _():
                top_flows[s].send(tiles - 1, tile_ref)

            pltpu.make_async_copy(
                tile_ref.at[pl.ds(0, width)], top.at[pl.ds(s * width, width)], local_sem.at[4]
            ).start()

    def lanes(count):
        return lax.broadcasted_iota(jnp.int32, (1, count), 1).astype(F32)

    def column(start, rows=step_rows):
        ids = lax.broadcasted_iota(jnp.int32, (rows, 1), 0)
        return (ids + start).astype(F32)

    def pivot_row(s):
        return pivot[pl.ds(s, 1), :].astype(F32)

    def undo(rows, upto):
        for s in reversed(range(upto)):
            listed = pivot_row(s)
            shift = lanes(width) + F32(s * width) - listed
            moved = jnp.where(rows == listed, shift, F32(0))
            rows = rows + jnp.sum(moved, axis=1, keepdims=True)
        return rows

    def one_hot(rows, ids):
        return jnp.where(rows == ids, F32(1), F32(0)).astype(BF16)

    load_pivots.wait()
    load_tile.wait()

    def cut_tile(i, carry):
        at = pl.ds(pl.multiple_of(i * step_rows, step_rows), step_rows)
        for k, part in enumerate(split3(first[at, :])):
            parts[k, at, :] = part
        return carry

    lax.fori_loop(0, tiles * blocks, cut_tile, 0)

    def pick_copy(s, slot, where, device):
        return pltpu.make_async_remote_copy(
            src_ref=picked.at[s],
            dst_ref=picked_in.at[s, slot],
            send_sem=pick_send.at[s, where],
            recv_sem=pick_recv.at[s, slot],
            device_id=device,
            device_id_type=MESH,
        )

    partner = {"prow": x * CORES + (CORES - 1 - core)}
    held_ids = jnp.concatenate(
        [
            lanes(width) + ((block * prow_count + prow) * width).astype(F32)
            for block in range(blocks)
        ],
        axis=1,
    )
    def pick_rows(s):
        def pick(i, carry):
            start = i * width
            at = pl.ds(pl.multiple_of(start, width), width)
            rows = jnp.sum(
                jnp.where(column(start, width) == lanes(width), pivot_row(s), F32(0)),
                axis=1, keepdims=True,
            )
            chosen = one_hot(undo(rows, s), held_ids)
            picked[s, at, :] = (
                dot(chosen, parts[2]) + dot(chosen, parts[1]) + dot(chosen, parts[0])
            )
            return carry

        lax.fori_loop(0, width // width, pick, 0)

        @pl.when(core != s % CORES)
        def _():
            pick_copy(s, 0, 0, partner).start()

    def add_in(s, slot):
        pick_copy(s, slot, 1, partner).wait_recv()

        def add(i, carry):
            at = pl.ds(pl.multiple_of(i * step_rows, step_rows), step_rows)
            picked[s, at, :] += picked_in[s, slot, at, :]
            return carry

        lax.fori_loop(0, tiles, add, 0)

    def pass_picked(s, when):
        owner = s // CORES

        @pl.when(both(core == s % CORES, x != owner, when))
        def _():
            add_in(s, 0)

            @pl.when(both(x < owner, x > 0))
            def _():
                add_in(s, 1)

            @pl.when(both(x > owner, x < chips - 1))
            def _():
                add_in(s, 2)

            @pl.when(x < owner)
            def _():
                pick_copy(s, 1, 1, {"prow": prow + CORES}).start()

            @pl.when(x > owner)
            def _():
                pick_copy(s, 2, 1, {"prow": prow - CORES}).start()

    def urgent(s):
        return pcol > 0 if s == 0 else pcol == 0

    def pick_all(order):
        for s in order:
            pick_rows(s)
            pass_picked(s, urgent(s))

    @pl.when(pcol == 0)
    def _():
        pick_all([*range(1, sections), 0])

    @pl.when(pcol > 0)
    def _():
        pick_all([*range(sections)])

    for s in range(sections):

        @pl.when(both(prow == s, waits_for_picks(s)))
        def _(s=s):
            top_flows[s].send(tiles - 1, tile_ref)


    @pl.when(owns_row)
    def _():
        pltpu.make_async_copy(lower_ref.at[prow], low_in, local_sem.at[2]).wait()

        def prepare(i, carry):
            start = i * step_rows
            at = pl.ds(pl.multiple_of(start, step_rows), step_rows)
            below = column(start) > lanes(width)
            same = column(start) == lanes(width)
            unit = jnp.where(below, low_in[at, :], jnp.where(same, F32(1), F32(0)))
            low_wide[at, :] = wide(unit)
            return carry

        lax.fori_loop(0, tiles, prepare, 0)

    def stack(ref, i, value):
        high, low = split2(value)
        start = i * step_rows
        for k, part in enumerate((high, low, high)):
            at = pl.ds(pl.multiple_of(k * width + start, step_rows), step_rows)
            ref[at, :] = part

    @pl.when(owns_col)
    def _():
        pltpu.make_async_copy(upper_ref.at[pcol], up_in, local_sem.at[3]).wait()

        def prepare(i, carry):
            start = i * step_rows
            at = pl.ds(pl.multiple_of(start, step_rows), step_rows)
            kept = jnp.where(column(start) <= lanes(width), up_in[at, :], F32(0))
            stack(up_stack, i, kept)
            return carry

        lax.fori_loop(0, tiles, prepare, 0)

    def take_picked(s):
        owner = s // CORES
        add_in(s, 0)
        slots = [1] * (owner > 0) + [2] * (owner < chips - 1)
        for slot in slots[:-1]:
            add_in(s, slot)
        for slot in slots[-1:]:
            pick_copy(s, slot, 1, partner).wait_recv()

        def put(i, carry):
            at = pl.ds(pl.multiple_of(i * step_rows, step_rows), step_rows)
            value = picked[s, at, :]
            for slot in slots[-1:]:
                value = value + picked_in[s, slot, at, :]
            out_ref[at, :] = value
            return carry

        lax.fori_loop(0, tiles, put, 0)

    ways = grid_ways(pcol, pcol_count)
    plans = [[tree_plan(pcol_count, s, k) for k in range(2)] for s in range(sections)]
    sends = [[[among(pcol, who) for who in plan[2]] for plan in pair] for pair in plans]
    gets = [[among(pcol, plan[1]) for plan in pair] for pair in plans]

    def farthest(s, node):
        return max(plan[0][node] for plan in plans[s])

    def live(s):
        return jnp.where(prow > s, blocks, blocks - 1)

    def place_of(s, i):
        turn = lax.div(i, per_block)
        block = blocks - live(s) + turn
        return block * width + (i - turn * per_block) * span

    part_rows = relay_rows // PARTS

    def col_copy(s, k, i, h, way):
        start = place_of(s, i) + k * relay_rows + h * part_rows
        piece = pl.ds(pl.multiple_of(start, part_rows), part_rows)
        return pltpu.make_async_remote_copy(
            src_ref=col_panel.at[s, piece],
            dst_ref=col_panel.at[s, piece],
            send_sem=col_send.at[s, k, way],
            recv_sem=col_recv.at[s, k, i * PARTS + h],
            device_id=ways[way][1],
            device_id_type=MESH,
        )

    def col_start(s, k, i, h):
        for way in range(4):

            @pl.when(sends[s][k][way])
            def _(way=way):
                col_copy(s, k, i, h, way).start()

    def update(s, at):
        return out_ref[at, :] - dot(wide(col_panel[s, at, :]), row_stack[s])

    def rows_of(s, i):
        return pl.ds(pl.multiple_of(place_of(s, i), span), span)

    def produce(s, i, value):
        at = rows_of(s, i)
        value = dot(wide(value), up_stack[...])
        col_panel[s, at, :] = value
        out_ref[at, :] = value

    def start_both(s, i):
        for h in range(PARTS):
            for k in range(2):
                col_start(s, k, i, h)

    def produce_first(start, stop):
        def body(i, carry):
            produce(0, i, out_ref[rows_of(0, i), :])

            @pl.when(i > start)
            def _():
                start_both(0, i - 1)

            return carry

        lax.fori_loop(start, stop, body, 0)
        start_both(0, stop - 1)

    for s in range(1, min(CORES, sections)):

        @pl.when(both(pcol == 0, prow == s))
        def _(s=s):
            take_picked(s)
            produce_first(0, per_block)
            pl.semaphore_signal(gate, inc=1, device_id=partner, device_id_type=MESH)

    def row_product(s, chunk):
        at = pl.ds(chunk * step_rows, step_rows)
        stack(core_stack, chunk, out_ref[at, :])
        upto = (chunk + 1) * step_rows
        value = F32(0)
        for k in range(3):
            upper = pl.ds(k * width, upto)
            value = value + dot(low_wide[at, k * width : k * width + upto], core_stack[upper, :])
        row_panel[s, at, :] = value
        out_ref[at, :] = value

    @pl.when(both(prow == 0, pcol > 0))
    def _():
        take_picked(0)
        for chunk in range(tiles):
            row_product(0, chunk)
            if chunk > 0:
                row_flows[0].send(chunk - 1, row_panel.at[0])
        row_flows[0].send(tiles - 1, row_panel.at[0])

    later = both(prow > 0, prow < min(CORES, sections), pcol > 0)

    def land_tops():
        for s in range(sections):

            @pl.when(prow == s)
            def _(s=s):
                pltpu.make_async_copy(
                    tile_ref.at[pl.ds(0, width)], top.at[pl.ds(s * width, width)], local_sem.at[4]
                ).wait()

        for chunk in range(tiles):
            for flow in top_flows:
                flow.pass_on(chunk)
            if chunk == tiles - 2:
                for s in range(sections):
                    pass_picked(s, jnp.logical_not(urgent(s)))

            def cut_top(s, carry, chunk=chunk):
                start = s * width + chunk * step_rows
                at = pl.ds(pl.multiple_of(start, step_rows), step_rows)
                for k, part in enumerate(split3(top[at, :])):
                    top_parts[k, at, :] = part
                return carry

            lax.fori_loop(0, sections, cut_top, 0)

    pl.when(jnp.logical_not(later))(land_tops)

    def settle(block, first_part=0, parts_count=1, size=width):
        def place(i, carry):
            start = i * size
            at = pl.ds(pl.multiple_of(block * width + start, size), size)
            rows = column(start + (block * prow_count + prow) * width, size)
            rows = undo(rows, sections)
            chosen = one_hot(rows, lanes(sections * width))
            value = (
                dot(chosen, top_parts[2]) + dot(chosen, top_parts[1]) + dot(chosen, top_parts[0])
            )
            out_ref[at, :] = jnp.where(rows < F32(sections * width), value, first[at, :])
            return carry

        lax.fori_loop(first_part, first_part + parts_count, place, 0)

    def forwards(s):
        return both(core == s % CORES, prow != s)

    def pass_row(s):
        for chunk in range(tiles):
            row_flows[s].pass_on(chunk)

    def take_row(s):
        @pl.when(jnp.logical_not(forwards(s)))
        def _():
            pass_row(s)

        def cut(i, carry):
            at = pl.ds(pl.multiple_of(i * step_rows, step_rows), step_rows)
            stack(row_stack.at[s], i, row_panel[s, at, :])
            return carry

        lax.fori_loop(0, tiles, cut, 0)

    @pl.when(pcol == 0)
    def _():
        @pl.when(jnp.logical_not(owns_row))
        def _():
            for half in range(2):
                settle(0, half, 1, width // 2)
                produce_first(half * per_block // 2, (half + 1) * per_block // 2)

        for block in range(1, blocks):
            settle(block)
        for s in range(CORES, sections):

            @pl.when(prow == s)
            def _(s=s):
                take_picked(s)

        if sections > 1:

            @pl.when(prow == 0)
            def _():
                pl.semaphore_wait(gate, 1)

        paired = [s for s in range(CORES, sections) if s ^ 1 >= sections]
        for s in paired:

            @pl.when(prow == s ^ 1)
            def _():
                pl.semaphore_wait(gate, 1)

        for s in paired:

            @pl.when(prow == s)
            def _():
                produce_first(0, per_block + per_block // 3)
                pl.semaphore_signal(gate, inc=1, device_id=partner, device_id_type=MESH)

        done = jnp.where(both(prow > 0, prow < CORES) | jnp.logical_not(owns_row), per_block, 0)
        for s in paired:
            done = jnp.where(prow == s, per_block + per_block // 3, done)
        produce_first(done, live(0) * per_block)

    @pl.when(both(pcol > 0, jnp.logical_not(later)))
    def _():
        for block in range(1, blocks):
            settle(block)

        @pl.when(jnp.logical_not(owns_row))
        def _():
            settle(0)

    begin, begin_of, lates, computes, counts = jnp.int32(0), [], [], [], []
    forward_at = []
    for s in range(sections):
        counts.append(live(s) * per_block)
        begin_of.append(begin)
        lates.append(
            [begin + pick_static(pcol, {n: HOP * h for n, h in plan[0].items()}) for plan in plans[s]]
        )
        lag = {n: HOP * farthest(s, n) + (LAG if n != s + 1 else 0) for n in range(pcol_count)}
        slack = jnp.where(x == 0, per_block, 0) if s == 0 else 0
        rest = PATIENCE if s == 0 else 0
        wait = jnp.where(both(prow >= CORES, prow < sections, pcol != 1), rest, 0)
        early = {n: HOP * farthest(s, n) - EARLY[min(s, 1)] for n in range(pcol_count)}
        forward_at.append(begin + pick_static(pcol, early))
        computes.append(begin + pick_static(pcol, lag) + jnp.where(pcol == s + 1, slack, wait))
        if s + 1 < sections:
            begin = begin + HOP * farthest(s, s + 1) + 1 + slack
            begin = begin + jnp.where(prow == s + 1, per_block, 0)
            for n in range(s + 2, pcol_count):
                ahead = HOP * (farthest(s, s + 1) + farthest(s + 1, n) - farthest(s, n))
                assert ahead + 1 >= (LAG if n == s + 2 else 0) + rest

    def inline(s):
        return pcol < 0 if s + 1 == sections else pcol > s

    def compute(s, j):
        last = s + 1 == sections
        skip = 0 if last else counts[s] - counts[s + 1]

        @pl.when(j == 0)
        def _():
            if s == 0:
                for other in range(1, sections):

                    @pl.when(prow == other)
                    def _(other=other):
                        take_picked(other)

            take_row(s)

        if s == 0:

            @pl.when(both(later, j == per_block))
            def _():
                land_tops()
                for block in range(1, blocks):
                    settle(block)

        at = rows_of(s, j)
        value = update(s, at)
        if last:
            out_ref[at, :] = value
            return
        makes = both(pcol == s + 1, j >= skip)

        @pl.when(jnp.logical_not(makes))
        def _():
            out_ref[at, :] = value

        @pl.when(makes)
        def _():
            produce(s + 1, j - skip, value)

        per_tile = per_block // tiles
        for chunk in range(tiles):
            ready = (chunk + 1) * per_tile - 1

            @pl.when(both(prow == s + 1, pcol > s + 1, j == ready))
            def _(chunk=chunk):
                row_product(s + 1, chunk)
                if chunk == tiles - 1:
                    row_flows[s + 1].send(chunk, row_panel.at[s + 1])

            if chunk < tiles - 1:

                @pl.when(both(prow == s + 1, pcol > s + 1, j == ready + 1))
                def _(chunk=chunk):
                    row_flows[s + 1].send(chunk, row_panel.at[s + 1])

    def turn(t, carry):
        for s in range(sections):
            for k in range(2):
                i = t - lates[s][k]

                @pl.when(both(gets[s][k], i >= 0, i < counts[s]))
                def _(s=s, k=k, i=i):
                    for h in range(PARTS):
                        col_copy(s, k, i, h, 0).wait_recv()
                        col_start(s, k, i, h)

            @pl.when(both(inline(s), forwards(s), t == jnp.maximum(forward_at[s], 0)))
            def _(s=s):
                pass_row(s)

            if s > 0:
                i = t - begin_of[s]

                @pl.when(both(pcol == s, i >= 0, i < counts[s]))
                def _(s=s, i=i):
                    start_both(s, i)

            j = t - computes[s]

            @pl.when(both(inline(s), j >= 0, j < counts[s]))
            def _(s=s, j=j):
                compute(s, j)

        return carry

    stop = jnp.int32(0)
    for s in range(sections):
        stop = jnp.maximum(stop, jnp.where(inline(s), computes[s] + counts[s], 0))
        for k in range(2):
            stop = jnp.maximum(stop, jnp.where(gets[s][k], lates[s][k] + counts[s], 0))
        if s > 0:
            stop = jnp.maximum(stop, jnp.where(pcol == s, begin_of[s] + counts[s], 0))
    lax.fori_loop(0, stop, turn, 0)
    last = sections - 1

    @pl.when(both(prow == 0, pcol == 0))
    def _():
        take_picked(0)

    @pl.when(both(pcol > last, jnp.logical_not(inline(last))))
    def _():
        @pl.when(forwards(last))
        def _():
            pass_row(last)

        take_row(last)

    def save(block):
        at = pl.ds(block * width, width)
        return pltpu.make_async_copy(out_ref.at[at], final_ref.at[at], local_sem.at[block])

    for block in range(blocks):

        @pl.when(both(pcol > last, block >= blocks - live(last)))
        def _(block=block):
            at = pl.ds(block * width, width)
            out_ref[at, :] = update(last, at)

        save(block).start()

    for s in range(sections):
        top_flows[s].finish(tiles)

        @pl.when(pcol > s)
        def _(s=s):
            row_flows[s].finish(tiles)

        owner = s // CORES

        @pl.when(core != s % CORES)
        def _(s=s):
            pick_copy(s, 0, 0, partner).wait_send()

        @pl.when(both(core == s % CORES, x != owner))
        def _(s=s):
            pick_copy(s, 0, 1, partner).wait_send()

        for k in range(2):
            for way in range(4):
                for count in (blocks - 1, blocks):

                    @pl.when(both(sends[s][k][way], live(s) == count))
                    def _(s=s, k=k, way=way, count=count):
                        piece = pl.ds(0, count * width // 2)
                        pltpu.make_async_remote_copy(
                            src_ref=col_panel.at[s, piece],
                            dst_ref=col_panel.at[s, piece],
                            send_sem=col_send.at[s, k, way],
                            recv_sem=col_recv.at[s, k, 0],
                            device_id=ways[way][1],
                            device_id_type=MESH,
                        ).wait_send()

    for block in range(blocks):
        save(block).wait()


def on_device(matrix, pivots, lower_inv, upper_inv):
    prow_count = lax.axis_size("prow")
    pcol_count = lax.axis_size("pcol")
    tile = matrix[0, 0]
    rows, width = tile.shape
    sections = pivots.shape[0]
    blocks = rows // width
    assert width == pivots.shape[1] and sections <= prow_count and sections <= pcol_count
    tiles = 3
    relays = blocks * 6
    dma = pltpu.SemaphoreType.DMA
    args = (tile, pivots, lower_inv, upper_inv)
    out = pl.pallas_call(
        functools.partial(factor_kernel, prow_count, pcol_count, sections, width, blocks),
        out_shape=jax.ShapeDtypeStruct(tile.shape, tile.dtype),
        in_specs=[pl.BlockSpec(memory_space=pl.ANY)] * 4,
        out_specs=pl.BlockSpec(memory_space=pl.ANY),
        scratch_shapes=[
            pltpu.VMEM((rows, width), F32),
            pltpu.VMEM((rows, width), F32),
            pltpu.VMEM(pivots.shape, jnp.int32),
            pltpu.VMEM((width, width), F32),
            pltpu.VMEM((width, width), F32),
            pltpu.VMEM((3, rows, width), BF16),
            pltpu.VMEM((sections * width, width), F32),
            pltpu.VMEM((3, sections * width, width), BF16),
            pltpu.VMEM((sections, width, width), F32),
            pltpu.VMEM((sections, 3, width, width), F32),
            pltpu.VMEM((sections, width, width), F32),
            pltpu.VMEM((sections, rows, width), F32),
            pltpu.VMEM((sections, 3 * width, width), BF16),
            pltpu.VMEM((width, 3 * width), BF16),
            pltpu.VMEM((3 * width, width), BF16),
            pltpu.VMEM((3 * width, width), BF16),
            dma((4 + blocks,)),
            dma((sections, 3)),
            dma((sections, tiles)),
            dma((sections, 2)),
            dma((sections, 3)),
            dma((sections, 3)),
            dma((sections, tiles)),
            dma((sections, 2, 4)),
            dma((sections, 2, relays * PARTS)),
            pltpu.SemaphoreType.REGULAR,
        ],
        compiler_params=pltpu.CompilerParams(
            collective_id=0, has_side_effects=True, vmem_limit_bytes=40 * 1024 * 1024
        ),
    )(*[pltpu.with_memory_space_constraint(v, pltpu.HBM) for v in args])
    return out[None, None]


def solution(mesh):
    return jax.shard_map(
        on_device,
        mesh=mesh,
        in_specs=(P("prow", "pcol", None, None), P(), P(), P()),
        out_specs=P("prow", "pcol", None, None),
        check_vma=False,
    )
```
